256 devices in a mesh: section: 8 (over y, core), gx: 8 (over z), gy: 4 (over x).
Axes of the slice: x: 4, y: 4, z: 8, core: 2. Of those that a mesh axis runs over, the one named last changes fastest.
Arguments:
- load_index: int32 [8], P('section'), may hold values from 0 to 63
- load_table: float32 [64, 3], replicated, may hold values from -4 to 4
- toughness: float32 [8, 128, 64, 128], P('section', 'gx', 'gy'), may hold values from 0.3 to 3
- clamp_mask: int32 [128, 64, 128], P('gx', 'gy'), may hold values 0 or 1
- load_mask: int32 [128, 64, 128], P('gx', 'gy'), may hold values 0 or 1
- crack_mask: int32 [128, 64, 128], P('gx', 'gy'), may hold values 0 or 1
Outputs:
- displacement: float32 [8, 3, 128, 64, 128], P('section', None, 'gx', 'gy')
- damage: float32 [8, 128, 64, 128], P('section', 'gx', 'gy')
- section_residuals: float32 [8, 8], P('section')
The draws below stay inside these ranges and needn't reach their ends.
All inputs are finite; a program needn't handle non-finite values. No bound on the sum of `clamp_mask` or of `load_mask` or of `crack_mask` on one device may be relied on, other than what follows from the above.
Results may differ from the reference program's by a relative error of at most 0.0003.
Values sent between devices are 32-bit elements; how exact they have to be, the bound alone decides.
No kernel may reach another device: no remote copies, remote signals or barrier semaphores. Data moves between devices by JAX's collectives and lax.ppermute only.
A program may use at most 64 MiB of HBM per device.

```python
import math
import jax
import jax.numpy as jnp
from jax import lax

CASE_DEV = 1
LOADS = 64
CASES = 8
SECTIONS = 8
NX = 128
NY = 64
NZ = 128
N_SECTION = 8


def with_ends(array, rng, low, high):
    dims = array.shape
    spot = [jax.random.randint(jax.random.fold_in(rng, axis), (), 0, dims[axis]) for axis in range(len(dims))]
    array = array.at[tuple(spot)].set(low)
    longest = dims.index(max(dims))
    spot[longest] = (spot[longest] + 1) % dims[longest]
    return array.at[tuple(spot)].set(high)


def steps_of(key, dims, cuts, least, high):
    def one(position, blocks):
        heights = jax.random.uniform(jax.random.fold_in(jax.random.fold_in(key, 6), position), (blocks,), jnp.float32, least / len(cuts), high / len(cuts))
        return jnp.repeat(jnp.exp(heights), dims[position] // blocks).reshape((-1,) + (1,) * (len(dims) - position - 1))

    level = one(*cuts[0])
    for cut in cuts[1:]:
        level = level * one(*cut)
    return level


def centred(stream_key, dims, scale, most, kind=jnp.bfloat16):
    values = jax.random.normal(stream_key, dims, jnp.float32) * scale
    return jnp.minimum(jnp.maximum(values, -most), most).astype(kind)


def setup_inputs(seed: int = 0) -> dict:
    keys = jax.random.split(jax.random.key(seed), 7)
    return {
        "load_index": with_ends(jax.random.randint(keys[0], (CASES,), 0, LOADS), jax.random.fold_in(keys[0], 1), 0, LOADS - 1).astype(jnp.int32),
        "load_table": centred(keys[1], (LOADS, 3), 1.0, 4.0, jnp.float32),
        "toughness": jnp.clip(jnp.exp(math.log(3.0) - 2.3025851 * jax.random.uniform(keys[2], (SECTIONS, NX, NY, NZ), jnp.float32) ** steps_of(keys[2], (SECTIONS, NX, NY, NZ), ((0, 8), (1, 8), (2, 4)), -0.2, 0.2)), 0.3, 3.0),
        "clamp_mask": with_ends((jax.random.randint(keys[3], (NX, NY, NZ), 0, 8) < 1).astype(jnp.int32), jax.random.fold_in(keys[3], 1), 0, 1),
        "load_mask": with_ends((jax.random.randint(keys[4], (NX, NY, NZ), 0, 8) < 1).astype(jnp.int32), jax.random.fold_in(keys[4], 1), 0, 1),
        "crack_mask": with_ends((jax.random.randint(keys[5], (NX, NY, NZ), 0, 32) < 1).astype(jnp.int32), jax.random.fold_in(keys[5], 1), 0, 1),
    }


lame_lambda = 1.0
shear_modulus = 1.0
relax_weight = 0.6
stiff_floor = 0.001
eigen_guard = 1e-08
neighbour_offsets = ((1, 0, 0), (-1, 0, 0), (0, 1, 0), (0, -1, 0), (0, 0, 1), (0, 0, -1))

def unit_offset(axis_index, sign):
    return tuple((sign if other == axis_index else 0 for other in range(3)))

def shifted(padded, offset):
    span_first = padded.shape[-3] - 2
    span_second = padded.shape[-2] - 2
    span_third = padded.shape[-1] - 2
    return padded[..., 1 + offset[0]:1 + offset[0] + span_first, 1 + offset[1]:1 + offset[1] + span_second, 1 + offset[2]:1 + offset[2] + span_third]

def component(field, index):
    return field[..., index, :, :, :]

def elastic_parts(moved_pad, damage_pad):
    stiff_pad = jnp.square(1.0 - damage_pad) + stiff_floor
    centre = shifted(stiff_pad, (0, 0, 0))
    current = shifted(moved_pad, (0, 0, 0))
    laplace = jnp.zeros_like(current)
    weights = jnp.zeros_like(centre)
    for offset in neighbour_offsets:
        face = 0.5 * (centre + shifted(stiff_pad, offset))
        weights = weights + face
        laplace = laplace + jnp.expand_dims(face, -4) * (shifted(moved_pad, offset) - current)
    divergence = jnp.zeros_like(centre)
    pairs = []
    for axis_index in range(3):
        forward = unit_offset(axis_index, 1)
        backward = unit_offset(axis_index, -1)
        part = component(moved_pad, axis_index)
        divergence = divergence + 0.5 * (shifted(part, forward) - shifted(part, backward))
        pairs.append(shifted(stiff_pad, forward) + shifted(stiff_pad, backward))
    flow = centre * divergence
    diagonal = shear_modulus * jnp.expand_dims(weights, -4) + 0.25 * (lame_lambda + shear_modulus) * jnp.stack(pairs, axis=-4)
    return (current, laplace, flow, diagonal)

def flow_gradient(flow_pad):
    parts = [0.5 * (shifted(flow_pad, unit_offset(axis_index, 1)) - shifted(flow_pad, unit_offset(axis_index, -1))) for axis_index in range(3)]
    return jnp.stack(parts, axis=-4)

def spectral_energy(strain_xx, strain_yy, strain_zz, strain_xy, strain_xz, strain_yz):
    middle_value = (strain_xx + strain_yy + strain_zz) / 3.0
    dev_xx = strain_xx - middle_value
    dev_yy = strain_yy - middle_value
    dev_zz = strain_zz - middle_value
    shear_sum = jnp.square(strain_xy) + jnp.square(strain_xz) + jnp.square(strain_yz)
    spread = jnp.square(dev_xx) + jnp.square(dev_yy) + jnp.square(dev_zz) + 2.0 * shear_sum
    radius = jnp.sqrt(spread / 6.0)
    guarded = spread / 6.0 + eigen_guard
    determinant = dev_xx * (dev_yy * dev_zz - jnp.square(strain_yz)) - strain_xy * (strain_xy * dev_zz - strain_yz * strain_xz) + strain_xz * (strain_xy * strain_yz - dev_yy * strain_xz)
    ratio = jnp.clip(determinant / (2.0 * guarded * jnp.sqrt(guarded)), -1.0, 1.0)
    angle = jnp.arccos(ratio) / 3.0
    largest = middle_value + 2.0 * radius * jnp.cos(angle)
    smallest = middle_value + 2.0 * radius * jnp.cos(angle + 2.0 * jnp.pi / 3.0)
    between = 3.0 * middle_value - largest - smallest
    positive = jnp.square(jax.nn.relu(largest)) + jnp.square(jax.nn.relu(between)) + jnp.square(jax.nn.relu(smallest))
    return 0.5 * lame_lambda * jnp.square(jax.nn.relu(3.0 * middle_value)) + shear_modulus * positive

def damage_update(moved_pad, damage_pad, toughness_cell, crack_cell):
    grads = [[0.5 * (shifted(component(moved_pad, first), unit_offset(second, 1)) - shifted(component(moved_pad, first), unit_offset(second, -1))) for second in range(3)] for first in range(3)]
    energy = spectral_energy(grads[0][0], grads[1][1], grads[2][2], 0.5 * (grads[0][1] + grads[1][0]), 0.5 * (grads[0][2] + grads[2][0]), 0.5 * (grads[1][2] + grads[2][1]))
    beside_all = jnp.zeros_like(energy)
    for offset in neighbour_offsets:
        beside_all = beside_all + shifted(damage_pad, offset)
    updated = (2.0 * energy + toughness_cell * beside_all) / (toughness_cell + 2.0 * energy + 6.0 * toughness_cell)
    return jnp.where(crack_cell > 0.5, 1.0, updated)

def pad_all(field):
    return jnp.pad(field, [(0, 0)] * (field.ndim - 3) + [(1, 1), (1, 1), (1, 1)])

def sweep(moved, damage, load_vector, toughness_cell, fixed, load, crack):
    damage_pad = pad_all(damage)
    current, laplace, flow, diagonal = elastic_parts(pad_all(moved), damage_pad)
    gradient = flow_gradient(pad_all(flow))
    residual = shear_modulus * laplace + (lame_lambda + shear_modulus) * gradient
    prescribed = load[None] * load_vector[:, None, None, None]
    relaxed = current + relax_weight * residual / diagonal
    new_moved = jnp.where(fixed[None] > 0.5, prescribed, relaxed)
    squares = jnp.sum((1.0 - fixed)[None] * jnp.square(residual))
    new_damage = damage_update(pad_all(new_moved), damage_pad, toughness_cell, crack)
    return (new_moved, new_damage, squares)

def reference(load_index, load_table, toughness, clamp_mask, load_mask, crack_mask):
    clamp = clamp_mask.astype(jnp.float32)
    load = load_mask.astype(jnp.float32)
    crack = crack_mask.astype(jnp.float32)
    fixed = jnp.maximum(clamp, load)
    cells = float(NX * NY * NZ)
    columns = jnp.arange(N_SECTION, dtype=jnp.int32)

    def one_case(item):
        case_index, table_row = item
        load_vector = load_table[table_row]
        home = (case_index // CASE_DEV).astype(jnp.int32)
        moved = load[None] * load_vector[:, None, None, None]
        norms = jnp.zeros((N_SECTION,), jnp.float32)

        def advance(round_index, carry):
            moved_now, damage_now, norms_now = carry
            section_index = ((home + round_index) % N_SECTION).astype(jnp.int32)
            field = lax.dynamic_index_in_dim(toughness, section_index, 0, keepdims=False)
            moved_next, damage_next, squares = sweep(moved_now, damage_now, load_vector, field, fixed, load, crack)
            entry = jnp.sqrt(squares / (3.0 * cells))
            norms_next = norms_now + (columns == section_index).astype(jnp.float32) * entry
            return (moved_next, damage_next, norms_next)
        return lax.fori_loop(0, N_SECTION, advance, (moved, crack, norms))
    moved, damage, norms = lax.map(one_case, (jnp.arange(CASES, dtype=jnp.int32), load_index))
    return (moved, damage, norms)
```

```python
import functools

import jax
import jax.numpy as jnp
from jax import lax
from jax.experimental import pallas as pl
from jax.experimental.pallas import tpu as pltpu
from jax.sharding import PartitionSpec as P

GROUPS = (4, 4)
B = 16
HALO = 2 * max(GROUPS) + 1
YP = B + 2 * HALO
ROWS = -(-(YP * YP + 16) // 8) * 8
H_OUT = 0.5 * (1.0 + 0.001)

COS_THIRD = (
    1.000000008260009, -0.22222426779181312, -0.06576120509434145, -0.035390736331322045,
    -0.012547845736683551, -0.050373368401680454, 0.05848138776830297, -0.07087101496233855,
)
SIN_THIRD = (
    1.1547005306829978, 0.1069186220087089, 0.04565984619644209, 0.027903402002033718,
    0.00953945386696008, 0.04580735112208377, -0.054824704413705544, 0.06541734748383539,
)

ROUNDS = sum(GROUPS)
PLACES = [(g, j) for g, k in enumerate(GROUPS) for j in range(k)]
T_HALO = [2 * (GROUPS[g] - 1 - j) for g, j in PLACES]
T_MAX = max(T_HALO)
VMEM = pl.BlockSpec(memory_space=pltpu.VMEM)
SMEM = pl.BlockSpec(memory_space=pltpu.SMEM)
f32 = jnp.float32


def rows_of(h):
    side = B + 2 * h
    return side * side if h == 0 else -(-(side * side + 8) // 8) * 8


def mask_widths():
    k = GROUPS[0]
    return (2 * k - 1, 2 * k + 1, 2 * k, T_MAX)


def state_widths(k):
    return (2 * k + 1,) * 3 + (2 * k,)


def tri(h):
    return h * (h - 1) // 2


def slab_rows(widths):
    return B * sum(widths)


def corner_rows(widths):
    return -(-sum(2 * tri(h) for h in widths) // 8) * 8


def pieces(n):
    return [(s, min(8, n - s)) for s in range(0, n, 8)]


def pack_slabs(readers, widths, outs):
    xhi, xlo, yhi, ylo = outs
    off = 0
    for read, w in zip(readers, widths):
        for l in range(w):
            for s, n in pieces(B):
                xhi[pl.ds(off + l * B + s, n), :] = read(B - w + l, s, n)
                xlo[pl.ds(off + l * B + s, n), :] = read(l, s, n)
        for x in range(B):
            for s, n in pieces(w):
                yhi[pl.ds(off + x * w + s, n), :] = read(x, B - w + s, n)
                ylo[pl.ds(off + x * w + s, n), :] = read(x, s, n)
        off += B * w


def corner_kernel(widths, xlo, xhi, yhi, ylo):
    off = o = 0
    for h in widths:
        for slab, layer in ((xlo, lambda a: h - a), (xhi, lambda a: a - 1)):
            for a in range(1, h):
                n = h - a
                base = off + layer(a) * B
                yhi[pl.ds(o, n), :] = slab[pl.ds(base + B - n, n), :]
                ylo[pl.ds(o, n), :] = slab[pl.ds(base, n), :]
                o += n
        off += B * h


def unpack(own, slabs, corners, widths, edges, stores, reach=None):
    xlo, xhi, ylo, yhi = slabs
    clo, chi = corners
    exlo, exhi, eylo, eyhi = edges
    off = o = 0
    for f, h in enumerate(widths):
        put = stores[f]
        for x in range(B):
            for s, n in pieces(B):
                put(x, s, own[f](x, s, n), None)
        for l in range(h):
            for s, n in pieces(B):
                put(l - h, s, xlo[pl.ds(off + l * B + s, n), :], exlo)
                put(B + l, s, xhi[pl.ds(off + l * B + s, n), :], exhi)
        for x in range(B):
            for s, n in pieces(h):
                put(x, s - h, ylo[pl.ds(off + x * h + s, n), :], eylo)
                put(x, B + s, yhi[pl.ds(off + x * h + s, n), :], eyhi)
        for side, edge in ((0, exlo), (1, exhi)):
            for a in range(1, h):
                n = h - a
                x = -a if side == 0 else B + a - 1
                put(x, -n, clo[pl.ds(o, n), :], jnp.logical_or(edge, eylo))
                put(x, B, chi[pl.ds(o, n), :], jnp.logical_or(edge, eyhi))
                o += n
        off += B * h


def edges_of(place):
    gx, gy = place[0], place[1]
    return gx == 0, gx == place[2] - 1, gy == 0, gy == place[3] - 1


def first_pack_kernel(clamp, load, crack, tough, *outs):
    def own(ref):
        return lambda x, y, n: ref[x, pl.ds(y, n), :].astype(f32)

    def fixed(x, y, n):
        return jnp.maximum(clamp[x, pl.ds(y, n), :], load[x, pl.ds(y, n), :]).astype(f32)

    readers = (fixed, own(load), own(crack), lambda x, y, n: tough[0, x, pl.ds(y, n), :])
    pack_slabs(readers, mask_widths(), outs)


def row(x, y):
    return (x + HALO) * YP + y + HALO


def load_vector(place, table):
    return [table[place[4], i] for i in range(3)]


def first_kernel(
    sides, place, table, clamp, load, crack, tough, xlo, xhi, ylo, yhi, clo, chi,
    state, fix, ld, cr, own_free, *tough_outs,
):
    w = load_vector(place, table)
    edges = edges_of(place)

    def own(ref):
        return lambda x, y, n: ref[x, pl.ds(y, n), :].astype(f32)

    def fixed(x, y, n):
        return jnp.maximum(clamp[x, pl.ds(y, n), :], load[x, pl.ds(y, n), :]).astype(f32)

    def choose(outside, value, other):
        return value if outside is None else jnp.where(outside, other, value)

    def put_fixed(x, y, v, outside):
        fix[pl.ds(row(x, y), v.shape[0]), :] = choose(outside, v, 1.0)
        if outside is None:
            own_free[pl.ds(row(x, y), v.shape[0]), :] = 1.0 - v

    def put_load(x, y, v, outside):
        v = choose(outside, v, 0.0)
        at = pl.ds(row(x, y), v.shape[0])
        ld[at, :] = v
        for i in range(3):
            state[i, at, :] = v * w[i]

    def put_crack(x, y, v, outside):
        at = pl.ds(row(x, y), v.shape[0])
        cr[at, :] = choose(outside, v, -1.0)
        state[3, at, :] = choose(outside, v, 0.0)

    def put_tough(x, y, v, outside):
        n = v.shape[0]
        for ref, h in zip(tough_outs, sides):
            lo, hi = max(y, -h), min(y + n, B + h)
            if -h <= x < B + h and lo < hi:
                at = (x + h) * (B + 2 * h) + lo + h
                ref[pl.ds(at, hi - lo), :] = v[lo - y : hi - y]

    own_free[...] = jnp.zeros_like(own_free)
    unpack(
        (fixed, own(load), own(crack), lambda x, y, n: tough[0, x, pl.ds(y, n), :]),
        (xlo, xhi, ylo, yhi), (clo, chi), mask_widths(), edges,
        (put_fixed, put_load, put_crack, put_tough),
    )


def horner(coefs, w):
    acc = w * coefs[-1] + coefs[-2]
    for c in coefs[-3::-1]:
        acc = acc * w + c
    return acc


def sweep(src, dst, half, flow, fix, ld, cr, own_free, tough, w, left):
    lane = lax.broadcasted_iota(jnp.int32, (8, 128), 1)
    first, last = lane == 0, lane == 127

    def up(v, outside=0.0):
        return jnp.where(last, outside, pltpu.roll(v, 127, 1))

    def down(v, outside=0.0):
        return jnp.where(first, outside, pltpu.roll(v, 1, 1))

    def over(h, body, carry=0):
        def one(i, c):
            for t in range(-(-(B + 2 * h) // 8)):
                c = body(i, (i - h + HALO) * YP + HALO - h + 8 * t, t, c)
            return c

        return lax.fori_loop(0, B + 2 * h, one, carry)

    def pass_flow(i, r, t, c):
        at = pl.ds(r, 8)
        keep = 1.0 - src[3, at, :]
        h = keep * keep * 0.5 + 0.0005
        z = src[2, at, :]
        div = (
            (src[0, pl.ds(r + YP, 8), :] - src[0, pl.ds(r - YP, 8), :])
            + (src[1, pl.ds(r + 1, 8), :] - src[1, pl.ds(r - 1, 8), :])
            + (up(z) - down(z))
        )
        half[at, :] = h
        flow[at, :] = jnp.where(cr[at, :] < -0.5, 0.0, h * div)
        return c

    def pass_moved(i, r, t, acc):
        at = pl.ds(r, 8)
        around = [pl.ds(r + d, 8) for d in (YP, -YP, 1, -1)]
        h0 = half[at, :]
        hn = [half[a, :] for a in around] + [up(h0, H_OUT), down(h0, H_OUT)]
        pairs = [hn[0] + hn[1], hn[2] + hn[3], hn[4] + hn[5]]
        weight = 6.0 * h0 + (pairs[0] + pairs[1] + pairs[2])
        faces = [h0 + n for n in hn]
        f0 = flow[at, :]
        slope = [
            flow[around[0], :] - flow[around[1], :],
            flow[around[2], :] - flow[around[3], :],
            up(f0) - down(f0),
        ]
        is_fixed = fix[at, :] > 0.5
        load = ld[at, :]
        squares = None
        for c in range(3):
            u0 = src[c, at, :]
            un = [src[c, a, :] for a in around] + [up(u0), down(u0)]
            res = slope[c] - weight * u0
            for f, n in zip(faces, un):
                res = res + f * n
            relaxed = u0 + (res * 0.6) / (weight + pairs[c])
            dst[c, at, :] = jnp.where(is_fixed, load * w[c], relaxed)
            squares = res * res if squares is None else squares + res * res
        return acc + jnp.where(own_free[at, :] > 0.5, squares, 0.0)

    def pass_damage(i, r, t, c):
        at = pl.ds(r, 8)
        g = []
        for k in range(3):
            v = dst[k, at, :]
            g.append(
                (
                    dst[k, pl.ds(r + YP, 8), :] - dst[k, pl.ds(r - YP, 8), :],
                    dst[k, pl.ds(r + 1, 8), :] - dst[k, pl.ds(r - 1, 8), :],
                    up(v) - down(v),
                )
            )
        total = g[0][0] + g[1][1] + g[2][2]
        third = total * (1.0 / 3.0)
        dx, dy, dz = g[0][0] - third, g[1][1] - third, g[2][2] - third
        xy, xz, yz = g[0][1] + g[1][0], g[0][2] + g[2][0], g[1][2] + g[2][1]
        xy2, xz2, yz2 = xy * xy, xz * xz, yz * yz
        spread = (dx * dx + dy * dy + dz * dz) + 0.5 * (xy2 + xz2 + yz2)
        det = dx * dy * dz + 0.25 * (xy * xz * yz - (dx * yz2 + dy * xz2 + dz * xy2))
        s6 = spread * (1.0 / 24.0)
        inv = lax.rsqrt(s6 + 1e-08)
        ratio = (det * 0.0625) * (inv * inv * inv)
        radius = s6 * lax.rsqrt(jnp.maximum(s6, 1e-37))
        wq = jnp.maximum(0.5 - 0.5 * jnp.abs(ratio), 0.0)
        cos = horner(COS_THIRD, wq)
        sin = (wq * lax.rsqrt(jnp.maximum(wq, 1e-37))) * horner(SIN_THIRD, wq)
        signed = jnp.where(ratio < 0.0, -radius, radius)
        a, b = signed * cos, signed * sin
        mean = total * (1.0 / 6.0)
        l1, rest = mean + 2.0 * a, mean - a
        p1, p2, p3 = jnp.maximum(l1, 0.0), jnp.maximum(rest + b, 0.0), jnp.maximum(rest - b, 0.0)
        trace = jnp.maximum(total, 0.0)
        psi2 = 0.25 * (trace * trace) + 2.0 * (p1 * p1 + p2 * p2 + p3 * p3)
        d0 = src[3, at, :]
        beside = (
            (src[3, pl.ds(r + YP, 8), :] + src[3, pl.ds(r - YP, 8), :])
            + (src[3, pl.ds(r + 1, 8), :] + src[3, pl.ds(r - 1, 8), :])
            + (up(d0) + down(d0))
        )
        gc = tough[pl.ds(i * (B + 2 * hd) + 8 * t, 8), :]
        new = (psi2 + gc * beside) / (psi2 + 7.0 * gc)
        kind = cr[at, :]
        dst[3, at, :] = jnp.where(kind > 0.5, 1.0, jnp.where(kind < -0.5, 0.0, new))
        return c

    hd = 2 * left
    over(hd + 2, pass_flow)
    acc = over(hd + 1, pass_moved, jnp.zeros((8, 128), f32))
    over(hd, pass_damage)
    return acc


def add_sum(sums, acc, r):
    lane = lax.broadcasted_iota(jnp.int32, (1, 128), 1)
    return jnp.where(lane % ROUNDS == r, jnp.sum(acc), sums)


def group_kernel(group, *refs):
    k = GROUPS[group]
    final = group == len(GROUPS) - 1
    refs = list(refs)

    def take(n):
        out = refs[:n]
        del refs[:n]
        return out

    place, table, fix, ld, cr, own_free = take(6)
    tough = take(k)
    w = load_vector(place, table)
    if group == 0:
        (src,) = take(1)
        sums = jnp.zeros((1, 128), f32)
    else:
        state, xlo, xhi, ylo, yhi, clo, chi, sums_in = take(8)
        sums = sums_in[...]
    if final:
        moved_out, damage_out, sums_out = take(3)
    else:
        (state_out,) = take(1)
        slab_outs = take(4)
        (sums_out,) = take(1)
    half, flow, *bufs = refs
    if group > 0:
        src = bufs[2]

        def own(f):
            return lambda x, y, n: state[f, x, pl.ds(y, n), :]

        def put(f):
            def one(x, y, v, outside):
                v = v if outside is None else jnp.where(outside, 0.0, v)
                src[f, pl.ds(row(x, y), v.shape[0]), :] = v

            return one

        unpack(
            [own(f) for f in range(4)], (xlo, xhi, ylo, yhi), (clo, chi), state_widths(k),
            edges_of(place), [put(f) for f in range(4)],
        )
    start = sum(GROUPS[:group])
    for j in range(k):
        dst = bufs[j % 2]
        acc = sweep(src, dst, half, flow, fix, ld, cr, own_free, tough[j], w, k - 1 - j)
        sums = add_sum(sums, acc, start + j)
        src = dst
    if final:
        for x in range(B):
            for s, n in pieces(B):
                at = pl.ds(row(x, s), n)
                for c in range(3):
                    moved_out[0, c, x, pl.ds(s, n), :] = src[c, at, :]
                damage_out[0, x, pl.ds(s, n), :] = src[3, at, :]
        sums_out[...] = jnp.broadcast_to(sums, sums_out.shape)
    else:
        for f in range(4):
            for x in range(B):
                for s, n in pieces(B):
                    state_out[f, x, pl.ds(s, n), :] = src[f, pl.ds(row(x, s), n), :]
        readers = [
            (lambda x, y, n, f=f: src[f, pl.ds(row(x, y), n), :]) for f in range(4)
        ]
        pack_slabs(readers, state_widths(GROUPS[group + 1]), slab_outs)
        sums_out[...] = sums


def table_kernel(scale, place, parts, out):
    total = jnp.sum(parts[...], axis=0, keepdims=True)
    root = jnp.sqrt(total * scale)
    out[...] = pltpu.roll(jnp.broadcast_to(root, (8, 128)), place[5], 1)[:1, :ROUNDS]


def call(kernel, name, outs, ins, scratch=(), smem=0, us=1.0):
    single = isinstance(outs, tuple)
    shapes = [outs] if single else outs
    res = pl.pallas_call(
        kernel,
        out_shape=[jax.ShapeDtypeStruct(s, f32) for s in shapes],
        in_specs=[SMEM] * smem + [VMEM] * (len(ins) - smem),
        out_specs=[VMEM] * len(shapes),
        scratch_shapes=list(scratch),
        name=name,
        compiler_params=pltpu.CompilerParams(vmem_limit_bytes=24 * 1024 * 1024),
        cost_estimate=pl.CostEstimate(
            flops=int(us * 4e6), bytes_accessed=int(us * 1e6), transcendentals=0
        ),
    )(*ins)
    return res[0] if single else res


def shift(x, axis, by):
    n = lax.axis_size(axis)
    return lax.ppermute(x, axis, [(i, (i + by) % n) for i in range(n)])


def swap_sides(slabs):
    xhi, xlo, yhi, ylo = slabs
    return shift(xhi, "gx", 1), shift(xlo, "gx", -1), shift(yhi, "gy", 1), shift(ylo, "gy", -1)


def swap_corners(xlo, xhi, widths, name):
    shape = (corner_rows(widths), 128)
    yhi, ylo = call(functools.partial(corner_kernel, widths), name, [shape] * 2, [xlo, xhi], us=0.3)
    return shift(yhi, "gy", 1), shift(ylo, "gy", -1)


def on_device(load_index, load_table, toughness, clamp_mask, load_mask, crack_mask):
    home = lax.axis_index("section").astype(jnp.int32)
    nx, ny = lax.axis_size("gx"), lax.axis_size("gy")
    place = jnp.stack(
        [
            lax.axis_index("gx").astype(jnp.int32),
            lax.axis_index("gy").astype(jnp.int32),
            jnp.int32(nx),
            jnp.int32(ny),
            load_index[0],
            home,
        ]
    )
    raw = [clamp_mask, load_mask, crack_mask, toughness]
    widths = mask_widths()
    slabs = call(first_pack_kernel, "first_pack", [(slab_rows(widths), 128)] * 4, raw, us=0.5)
    received = swap_sides(slabs)
    corners = swap_corners(received[0], received[1], widths, "first_corners")
    sides = tuple(sorted({h for h in T_HALO if h}, reverse=True))
    ext = (ROWS, 128)
    made = call(
        functools.partial(first_kernel, sides), "first",
        [(4,) + ext, ext, ext, ext, ext] + [(rows_of(h), 128) for h in sides],
        [place, load_table, *raw, *received, *corners], smem=2, us=1.0,
    )
    state, kinds = made[0], made[1:5]
    by_halo = dict(zip(sides, made[5:]))
    by_halo[0] = toughness.reshape(B * B, 128)
    tough = [
        by_halo[h] if r == 0 else shift(by_halo[h], "section", -r) for r, h in enumerate(T_HALO)
    ]
    sums = None
    for g, k in enumerate(GROUPS):
        start = sum(GROUPS[:g])
        ins = [place, load_table, *kinds, *tough[start : start + k]]
        if g == 0:
            ins.append(state)
        else:
            received = swap_sides(slabs)
            corners = swap_corners(received[0], received[1], state_widths(k), f"corners_{g}")
            ins += [state, *received, *corners, sums]
        final = g == len(GROUPS) - 1
        if final:
            outs = [(1, 3, B, B, 128), (1, B, B, 128), (nx * ny, 128)]
        else:
            n = slab_rows(state_widths(GROUPS[g + 1]))
            outs = [(4, B, B, 128)] + [(n, 128)] * 4 + [(1, 128)]
        scratch = [pltpu.VMEM(ext, f32)] * 2 + [pltpu.VMEM((4,) + ext, f32)] * (2 + (g > 0))
        res = call(
            functools.partial(group_kernel, g), f"group_{g}", outs, ins, scratch, smem=2, us=13.0
        )
        if final:
            moved, damage, parts = res
        else:
            state, slabs, sums = res[0], res[1:5], res[5]
    parts = lax.all_to_all(parts, ("gx", "gy"), 0, 0, tiled=True)
    scale = 1.0 / (3.0 * B * B * 128 * nx * ny)
    table = call(
        functools.partial(table_kernel, scale), "table", (1, ROUNDS), [place, parts], smem=1, us=0.1
    )
    return moved, damage, table


def solution(mesh):
    in_specs = (
        P("section"),
        P(),
        P("section", "gx", "gy", None),
        P("gx", "gy", None),
        P("gx", "gy", None),
        P("gx", "gy", None),
    )
    out_specs = (
        P("section", None, "gx", "gy", None),
        P("section", "gx", "gy", None),
        P("section", None),
    )
    return jax.shard_map(
        on_device, mesh=mesh, in_specs=in_specs, out_specs=out_specs, check_vma=False
    )
```

```python
import functools

import jax
import jax.numpy as jnp
from jax import lax
from jax.experimental import pallas as pl
from jax.experimental.pallas import tpu as pltpu
from jax.sharding import PartitionSpec as P

GROUPS = (4, 4)
B = 16
HALO = 2 * max(GROUPS) + 1
YP = B + 2 * HALO
ROWS = -(-(YP * YP + 16) // 8) * 8
H_OUT = 0.5 * (1.0 + 0.001)

COS_THIRD = (
    1.000000008260009, -0.22222426779181312, -0.06576120509434145, -0.035390736331322045,
    -0.012547845736683551, -0.050373368401680454, 0.05848138776830297, -0.07087101496233855,
)
SIN_THIRD = (
    1.1547005306829978, 0.1069186220087089, 0.04565984619644209, 0.027903402002033718,
    0.00953945386696008, 0.04580735112208377, -0.054824704413705544, 0.06541734748383539,
)

ROUNDS = sum(GROUPS)
PLACES = [(g, j) for g, k in enumerate(GROUPS) for j in range(k)]
T_HALO = [2 * (GROUPS[g] - 1 - j) for g, j in PLACES]
T_MAX = max(T_HALO)
VMEM = pl.BlockSpec(memory_space=pltpu.VMEM)
SMEM = pl.BlockSpec(memory_space=pltpu.SMEM)
f32 = jnp.float32


def rows_of(h):
    side = B + 2 * h
    return side * side if h == 0 else -(-(side * side + 8) // 8) * 8


def mask_widths():
    k = GROUPS[0]
    return (2 * k - 1, 2 * k + 1, 2 * k, T_MAX)


def state_widths(k):
    return (2 * k + 1,) * 3 + (2 * k,)


def tri(h):
    return h * (h - 1) // 2


def slab_rows(widths):
    return B * sum(widths)


def corner_rows(widths):
    return -(-sum(2 * tri(h) for h in widths) // 8) * 8


def pieces(n):
    return [(s, min(8, n - s)) for s in range(0, n, 8)]


def pack_slabs(readers, widths, outs):
    xhi, xlo, yhi, ylo = outs
    off = 0
    for read, w in zip(readers, widths):
        for l in range(w):
            for s, n in pieces(B):
                xhi[pl.ds(off + l * B + s, n), :] = read(B - w + l, s, n)
                xlo[pl.ds(off + l * B + s, n), :] = read(l, s, n)
        for x in range(B):
            for s, n in pieces(w):
                yhi[pl.ds(off + x * w + s, n), :] = read(x, B - w + s, n)
                ylo[pl.ds(off + x * w + s, n), :] = read(x, s, n)
        off += B * w


def corner_kernel(widths, xlo, xhi, yhi, ylo):
    off = o = 0
    for h in widths:
        for slab, layer in ((xlo, lambda a: h - a), (xhi, lambda a: a - 1)):
            for a in range(1, h):
                n = h - a
                base = off + layer(a) * B
                yhi[pl.ds(o, n), :] = slab[pl.ds(base + B - n, n), :]
                ylo[pl.ds(o, n), :] = slab[pl.ds(base, n), :]
                o += n
        off += B * h


def unpack(own, slabs, corners, widths, edges, stores, reach=None):
    xlo, xhi, ylo, yhi = slabs
    clo, chi = corners
    exlo, exhi, eylo, eyhi = edges
    off = o = 0
    for f, h in enumerate(widths):
        put = stores[f]
        for x in range(B):
            for s, n in pieces(B):
                put(x, s, own[f](x, s, n), None)
        for l in range(h):
            for s, n in pieces(B):
                put(l - h, s, xlo[pl.ds(off + l * B + s, n), :], exlo)
                put(B + l, s, xhi[pl.ds(off + l * B + s, n), :], exhi)
        for x in range(B):
            for s, n in pieces(h):
                put(x, s - h, ylo[pl.ds(off + x * h + s, n), :], eylo)
                put(x, B + s, yhi[pl.ds(off + x * h + s, n), :], eyhi)
        for side, edge in ((0, exlo), (1, exhi)):
            for a in range(1, h):
                n = h - a
                x = -a if side == 0 else B + a - 1
                put(x, -n, clo[pl.ds(o, n), :], jnp.logical_or(edge, eylo))
                put(x, B, chi[pl.ds(o, n), :], jnp.logical_or(edge, eyhi))
                o += n
        off += B * h


def edges_of(place):
    gx, gy = place[0], place[1]
    return gx == 0, gx == place[2] - 1, gy == 0, gy == place[3] - 1


def first_pack_kernel(clamp, load, crack, tough, *outs):
    def own(ref):
        return lambda x, y, n: ref[x, pl.ds(y, n), :].astype(f32)

    def fixed(x, y, n):
        return jnp.maximum(clamp[x, pl.ds(y, n), :], load[x, pl.ds(y, n), :]).astype(f32)

    readers = (fixed, own(load), own(crack), lambda x, y, n: tough[0, x, pl.ds(y, n), :])
    pack_slabs(readers, mask_widths(), outs)


def row(x, y):
    return (x + HALO) * YP + y + HALO


def load_vector(place, table):
    return [table[place[4], i] for i in range(3)]


def first_kernel(
    sides, place, table, clamp, load, crack, tough, xlo, xhi, ylo, yhi, clo, chi,
    state, fix, ld, cr, own_free, *tough_outs,
):
    w = load_vector(place, table)
    edges = edges_of(place)

    def own(ref):
        return lambda x, y, n: ref[x, pl.ds(y, n), :].astype(f32)

    def fixed(x, y, n):
        return jnp.maximum(clamp[x, pl.ds(y, n), :], load[x, pl.ds(y, n), :]).astype(f32)

    def choose(outside, value, other):
        return value if outside is None else jnp.where(outside, other, value)

    def put_fixed(x, y, v, outside):
        fix[pl.ds(row(x, y), v.shape[0]), :] = choose(outside, v, 1.0)
        if outside is None:
            own_free[pl.ds(row(x, y), v.shape[0]), :] = 1.0 - v

    def put_load(x, y, v, outside):
        v = choose(outside, v, 0.0)
        at = pl.ds(row(x, y), v.shape[0])
        ld[at, :] = v
        above, below = up(v), down(v)
        for i in range(3):
            state[i, at, :] = v * w[i]
            state[4 + i, at, :] = above * w[i]
            state[7 + i, at, :] = below * w[i]

    def put_crack(x, y, v, outside):
        at = pl.ds(row(x, y), v.shape[0])
        cr[at, :] = choose(outside, v, -1.0)
        put_state(state, 3, at, choose(outside, v, 0.0))

    def put_tough(x, y, v, outside):
        n = v.shape[0]
        for ref, h in zip(tough_outs, sides):
            lo, hi = max(y, -h), min(y + n, B + h)
            if -h <= x < B + h and lo < hi:
                at = (x + h) * (B + 2 * h) + lo + h
                ref[pl.ds(at, hi - lo), :] = v[lo - y : hi - y]

    own_free[...] = jnp.zeros_like(own_free)
    unpack(
        (fixed, own(load), own(crack), lambda x, y, n: tough[0, x, pl.ds(y, n), :]),
        (xlo, xhi, ylo, yhi), (clo, chi), mask_widths(), edges,
        (put_fixed, put_load, put_crack, put_tough),
    )


def horner(coefs, w):
    acc = w * coefs[-1] + coefs[-2]
    for c in coefs[-3::-1]:
        acc = acc * w + c
    return acc


def up(v, outside=0.0):
    lane = lax.broadcasted_iota(jnp.int32, v.shape, 1)
    return jnp.where(lane == 127, outside, pltpu.roll(v, 127, 1))


def down(v, outside=0.0):
    lane = lax.broadcasted_iota(jnp.int32, v.shape, 1)
    return jnp.where(lane == 0, outside, pltpu.roll(v, 1, 1))


def put_state(ref, f, at, v):
    ref[f, at, :] = v
    plus, minus = ((4 + f, 7 + f) if f < 3 else (10, 11))
    ref[plus, at, :] = up(v)
    ref[minus, at, :] = down(v)


def sweep(src, dst, half, flow, flow_z, fix, ld, cr, own_free, tough, w, left):
    def chunks(h, i):
        base = i * YP + HALO - h
        return [base + 8 * t for t in range(-(-(B + 2 * h) // 8))]

    def flow_row(i):
        done = []
        for r in chunks(hd + 2, i):
            at = pl.ds(r, 8)
            keep = 1.0 - src[3, at, :]
            h = keep * keep * 0.5 + 0.0005
            div = (
                (src[0, pl.ds(r + YP, 8), :] - src[0, pl.ds(r - YP, 8), :])
                + (src[1, pl.ds(r + 1, 8), :] - src[1, pl.ds(r - 1, 8), :])
                + (src[6, at, :] - src[9, at, :])
            )
            f = jnp.where(cr[at, :] < -0.5, 0.0, h * div)
            half[at, :] = h
            flow[at, :] = f
            done.append((at, up(f) - down(f)))
        return done

    def put_flow_z(done):
        for at, v in done:
            flow_z[at, :] = v

    def turned(ref, fields, h, i):
        out = []
        for r in chunks(h, i):
            at = pl.ds(r, 8)
            for f in fields:
                v = ref[f, at, :]
                plus, minus = ((4 + f, 7 + f) if f < 3 else (10, 11))
                out.append((plus, at, up(v)))
                out.append((minus, at, down(v)))
        return out

    def put_turned(ref, done):
        for f, at, v in done:
            ref[f, at, :] = v

    def half_of(d):
        keep = 1.0 - d
        return keep * keep * 0.5 + 0.0005

    def moved_row(i, acc):
        for r in chunks(hd + 1, i):
            at = pl.ds(r, 8)
            around = [pl.ds(r + d, 8) for d in (YP, -YP, 1, -1)]
            h0 = half[at, :]
            hn = [half[a, :] for a in around] + [half_of(src[10, at, :]), half_of(src[11, at, :])]
            pairs = [hn[0] + hn[1], hn[2] + hn[3], hn[4] + hn[5]]
            weight = 6.0 * h0 + (pairs[0] + pairs[1] + pairs[2])
            faces = [h0 + n for n in hn]
            slope = [
                flow[around[0], :] - flow[around[1], :],
                flow[around[2], :] - flow[around[3], :],
                flow_z[at, :],
            ]
            is_fixed = fix[at, :] > 0.5
            load = ld[at, :]
            squares = None
            for c in range(3):
                u0 = src[c, at, :]
                un = [src[c, a, :] for a in around] + [src[4 + c, at, :], src[7 + c, at, :]]
                res = slope[c] - weight * u0
                for f, n in zip(faces, un):
                    res = res + f * n
                relaxed = u0 + (res * 0.6) / (weight + pairs[c])
                dst[c, at, :] = jnp.where(is_fixed, load * w[c], relaxed)
                squares = res * res if squares is None else squares + res * res
            acc = acc + jnp.where(own_free[at, :] > 0.5, squares, 0.0)
        return acc

    def damage_row(i):
        for t, r in enumerate(chunks(hd, i)):
            at = pl.ds(r, 8)
            g = [
                (
                    dst[k, pl.ds(r + YP, 8), :] - dst[k, pl.ds(r - YP, 8), :],
                    dst[k, pl.ds(r + 1, 8), :] - dst[k, pl.ds(r - 1, 8), :],
                    dst[4 + k, at, :] - dst[7 + k, at, :],
                )
                for k in range(3)
            ]
            total = g[0][0] + g[1][1] + g[2][2]
            third = total * (1.0 / 3.0)
            dx, dy, dz = g[0][0] - third, g[1][1] - third, g[2][2] - third
            xy, xz, yz = g[0][1] + g[1][0], g[0][2] + g[2][0], g[1][2] + g[2][1]
            xy2, xz2, yz2 = xy * xy, xz * xz, yz * yz
            spread = (dx * dx + dy * dy + dz * dz) + 0.5 * (xy2 + xz2 + yz2)
            det = dx * dy * dz + 0.25 * (xy * xz * yz - (dx * yz2 + dy * xz2 + dz * xy2))
            s6 = spread * (1.0 / 24.0)
            inv = lax.rsqrt(s6 + 1e-08)
            ratio = (det * 0.0625) * (inv * inv * inv)
            radius = s6 * lax.rsqrt(jnp.maximum(s6, 1e-37))
            wq = jnp.maximum(0.5 - 0.5 * jnp.abs(ratio), 0.0)
            cos = horner(COS_THIRD, wq)
            sin = (wq * lax.rsqrt(jnp.maximum(wq, 1e-37))) * horner(SIN_THIRD, wq)
            signed = jnp.where(ratio < 0.0, -radius, radius)
            a, b = signed * cos, signed * sin
            mean = total * (1.0 / 6.0)
            l1, rest = mean + 2.0 * a, mean - a
            p1 = jnp.maximum(l1, 0.0)
            p2 = jnp.maximum(rest + b, 0.0)
            p3 = jnp.maximum(rest - b, 0.0)
            trace = jnp.maximum(total, 0.0)
            psi2 = 0.25 * (trace * trace) + 2.0 * (p1 * p1 + p2 * p2 + p3 * p3)
            beside = (
                (src[3, pl.ds(r + YP, 8), :] + src[3, pl.ds(r - YP, 8), :])
                + (src[3, pl.ds(r + 1, 8), :] + src[3, pl.ds(r - 1, 8), :])
                + (src[10, at, :] + src[11, at, :])
            )
            gc = tough[pl.ds((i - (HALO - hd)) * (B + 2 * hd) + 8 * t, 8), :]
            new = (psi2 + gc * beside) / (psi2 + 7.0 * gc)
            kind = cr[at, :]
            dst[3, at, :] = jnp.where(kind > 0.5, 1.0, jnp.where(kind < -0.5, 0.0, new))

    hd = 2 * left
    hm = hd + 1

    def first_loop(i, acc):
        later = turned(dst, range(3), hm, i - 1)
        flow_later = flow_row(i + 1)
        acc = moved_row(i, acc)
        put_turned(dst, later)
        put_flow_z(flow_later)
        return acc

    def second_loop(i, c):
        later = turned(dst, (3,), hd, i - 1) if left else ()
        damage_row(i)
        put_turned(dst, later)
        return c

    low, high = HALO - hm, HALO + B + hm
    put_flow_z(flow_row(low - 1))
    put_flow_z(flow_row(low))
    acc = lax.fori_loop(low, high, first_loop, jnp.zeros((8, 128), f32))
    put_turned(dst, turned(dst, range(3), hm, high - 1))
    low, high = HALO - hd, HALO + B + hd
    lax.fori_loop(low, high, second_loop, 0)
    if left:
        put_turned(dst, turned(dst, (3,), hd, high - 1))
    return acc


def add_sum(sums, acc, r):
    lane = lax.broadcasted_iota(jnp.int32, (1, 128), 1)
    return jnp.where(lane % ROUNDS == r, jnp.sum(acc), sums)


def group_kernel(group, *refs):
    k = GROUPS[group]
    final = group == len(GROUPS) - 1
    refs = list(refs)

    def take(n):
        out = refs[:n]
        del refs[:n]
        return out

    place, table, fix, ld, cr, own_free = take(6)
    tough = take(k)
    w = load_vector(place, table)
    if group == 0:
        (src,) = take(1)
        sums = jnp.zeros((1, 128), f32)
    else:
        state, xlo, xhi, ylo, yhi, clo, chi, sums_in = take(8)
        sums = sums_in[...]
    if final:
        moved_out, damage_out, sums_out = take(3)
    else:
        (state_out,) = take(1)
        slab_outs = take(4)
        (sums_out,) = take(1)
    half, flow, flow_z, *bufs = refs
    if group > 0:
        src = bufs[2]

        def own(f):
            return lambda x, y, n: state[f, x, pl.ds(y, n), :]

        def put(f):
            def one(x, y, v, outside):
                v = v if outside is None else jnp.where(outside, 0.0, v)
                put_state(src, f, pl.ds(row(x, y), v.shape[0]), v)

            return one

        unpack(
            [own(f) for f in range(4)], (xlo, xhi, ylo, yhi), (clo, chi), state_widths(k),
            edges_of(place), [put(f) for f in range(4)],
        )
    start = sum(GROUPS[:group])
    for j in range(k):
        dst = bufs[j % 2]
        acc = sweep(src, dst, half, flow, flow_z, fix, ld, cr, own_free, tough[j], w, k - 1 - j)
        sums = add_sum(sums, acc, start + j)
        src = dst
    if final:
        for x in range(B):
            for s, n in pieces(B):
                at = pl.ds(row(x, s), n)
                for c in range(3):
                    moved_out[0, c, x, pl.ds(s, n), :] = src[c, at, :]
                damage_out[0, x, pl.ds(s, n), :] = src[3, at, :]
        sums_out[...] = jnp.broadcast_to(sums, sums_out.shape)
    else:
        for f in range(4):
            for x in range(B):
                for s, n in pieces(B):
                    state_out[f, x, pl.ds(s, n), :] = src[f, pl.ds(row(x, s), n), :]
        readers = [
            (lambda x, y, n, f=f: src[f, pl.ds(row(x, y), n), :]) for f in range(4)
        ]
        pack_slabs(readers, state_widths(GROUPS[group + 1]), slab_outs)
        sums_out[...] = sums


def table_kernel(scale, place, parts, out):
    total = jnp.sum(parts[...], axis=0, keepdims=True)
    root = jnp.sqrt(total * scale)
    out[...] = pltpu.roll(jnp.broadcast_to(root, (8, 128)), place[5], 1)[:1, :ROUNDS]


def call(kernel, name, outs, ins, scratch=(), smem=0, us=1.0):
    single = isinstance(outs, tuple)
    shapes = [outs] if single else outs
    res = pl.pallas_call(
        kernel,
        out_shape=[jax.ShapeDtypeStruct(s, f32) for s in shapes],
        in_specs=[SMEM] * smem + [VMEM] * (len(ins) - smem),
        out_specs=[VMEM] * len(shapes),
        scratch_shapes=list(scratch),
        name=name,
        compiler_params=pltpu.CompilerParams(vmem_limit_bytes=32 * 1024 * 1024),
        cost_estimate=pl.CostEstimate(
            flops=int(us * 4e6), bytes_accessed=int(us * 1e6), transcendentals=0
        ),
    )(*ins)
    return res[0] if single else res


def shift(x, axis, by):
    n = lax.axis_size(axis)
    return lax.ppermute(x, axis, [(i, (i + by) % n) for i in range(n)])


def swap_sides(slabs):
    xhi, xlo, yhi, ylo = slabs
    return shift(xhi, "gx", 1), shift(xlo, "gx", -1), shift(yhi, "gy", 1), shift(ylo, "gy", -1)


def swap_corners(xlo, xhi, widths, name):
    shape = (corner_rows(widths), 128)
    yhi, ylo = call(functools.partial(corner_kernel, widths), name, [shape] * 2, [xlo, xhi], us=0.3)
    return shift(yhi, "gy", 1), shift(ylo, "gy", -1)


def on_device(load_index, load_table, toughness, clamp_mask, load_mask, crack_mask):
    home = lax.axis_index("section").astype(jnp.int32)
    nx, ny = lax.axis_size("gx"), lax.axis_size("gy")
    place = jnp.stack(
        [
            lax.axis_index("gx").astype(jnp.int32),
            lax.axis_index("gy").astype(jnp.int32),
            jnp.int32(nx),
            jnp.int32(ny),
            load_index[0],
            home,
        ]
    )
    raw = [clamp_mask, load_mask, crack_mask, toughness]
    widths = mask_widths()
    slabs = call(first_pack_kernel, "first_pack", [(slab_rows(widths), 128)] * 4, raw, us=0.5)
    received = swap_sides(slabs)
    corners = swap_corners(received[0], received[1], widths, "first_corners")
    sides = tuple(sorted({h for h in T_HALO if h}, reverse=True))
    ext = (ROWS, 128)
    made = call(
        functools.partial(first_kernel, sides), "first",
        [(12,) + ext, ext, ext, ext, ext] + [(rows_of(h), 128) for h in sides],
        [place, load_table, *raw, *received, *corners], smem=2, us=1.0,
    )
    state, kinds = made[0], made[1:5]
    by_halo = dict(zip(sides, made[5:]))
    by_halo[0] = toughness.reshape(B * B, 128)
    tough = [
        by_halo[h] if r == 0 else shift(by_halo[h], "section", -r) for r, h in enumerate(T_HALO)
    ]
    sums = None
    for g, k in enumerate(GROUPS):
        start = sum(GROUPS[:g])
        ins = [place, load_table, *kinds, *tough[start : start + k]]
        if g == 0:
            ins.append(state)
        else:
            received = swap_sides(slabs)
            corners = swap_corners(received[0], received[1], state_widths(k), f"corners_{g}")
            ins += [state, *received, *corners, sums]
        final = g == len(GROUPS) - 1
        if final:
            outs = [(1, 3, B, B, 128), (1, B, B, 128), (nx * ny, 128)]
        else:
            n = slab_rows(state_widths(GROUPS[g + 1]))
            outs = [(4, B, B, 128)] + [(n, 128)] * 4 + [(1, 128)]
        scratch = [pltpu.VMEM(ext, f32)] * 3 + [pltpu.VMEM((12,) + ext, f32)] * (2 + (g > 0))
        res = call(
            functools.partial(group_kernel, g), f"group_{g}", outs, ins, scratch, smem=2, us=13.0
        )
        if final:
            moved, damage, parts = res
        else:
            state, slabs, sums = res[0], res[1:5], res[5]
    parts = lax.all_to_all(parts, ("gx", "gy"), 0, 0, tiled=True)
    scale = 1.0 / (3.0 * B * B * 128 * nx * ny)
    table = call(
        functools.partial(table_kernel, scale), "table", (1, ROUNDS), [place, parts], smem=1, us=0.1
    )
    return moved, damage, table


def solution(mesh):
    in_specs = (
        P("section"),
        P(),
        P("section", "gx", "gy", None),
        P("gx", "gy", None),
        P("gx", "gy", None),
        P("gx", "gy", None),
    )
    out_specs = (
        P("section", None, "gx", "gy", None),
        P("section", "gx", "gy", None),
        P("section", None),
    )
    return jax.shard_map(
        on_device, mesh=mesh, in_specs=in_specs, out_specs=out_specs, check_vma=False
    )
```

```python
import functools

import jax
import jax.numpy as jnp
from jax import lax
from jax.experimental import pallas as pl
from jax.experimental.pallas import tpu as pltpu
from jax.sharding import PartitionSpec as P

GROUPS = (4, 4)
B = 16
HALO = 2 * max(GROUPS) + 1
YP = B + 2 * HALO
ROWS = -(-(YP * (YP + 1) + 32) // 8) * 8

COS_THIRD = (
    1.000000008260009, -0.22222426779181312, -0.06576120509434145, -0.035390736331322045,
    -0.012547845736683551, -0.050373368401680454, 0.05848138776830297, -0.07087101496233855,
)
SIN_THIRD = (
    1.1547005306829978, 0.1069186220087089, 0.04565984619644209, 0.027903402002033718,
    0.00953945386696008, 0.04580735112208377, -0.054824704413705544, 0.06541734748383539,
)

ROUNDS = sum(GROUPS)
SEGMENTS = ((0, 0, 1), (0, 1, 4), (1, 0, 4))
PLACES = [(g, j) for g, k in enumerate(GROUPS) for j in range(k)]
T_HALO = [2 * (GROUPS[g] - 1 - j) for g, j in PLACES]
T_MAX = max(T_HALO)
VMEM = pl.BlockSpec(memory_space=pltpu.VMEM)
SMEM = pl.BlockSpec(memory_space=pltpu.SMEM)
f32 = jnp.float32


def rows_of(h):
    side = B + 2 * h
    return side * side if h == 0 else -(-(side * side + 8) // 8) * 8


def mask_widths():
    k = GROUPS[0]
    return (2 * k - 1, 2 * k + 1, 2 * k, T_MAX)


def state_widths(k):
    return (2 * k + 1,) * 3 + (2 * k,)


def tri(h):
    return h * (h - 1) // 2


def slab_rows(widths):
    return B * sum(widths)


def corner_rows(widths):
    return -(-sum(2 * tri(h) for h in widths) // 8) * 8


def pieces(n):
    return [(s, min(8, n - s)) for s in range(0, n, 8)]


def pack_slabs(readers, widths, outs):
    xhi, xlo, yhi, ylo = outs
    off = 0
    for read, w in zip(readers, widths):
        for l in range(w):
            for s, n in pieces(B):
                xhi[pl.ds(off + l * B + s, n), :] = read(B - w + l, s, n)
                xlo[pl.ds(off + l * B + s, n), :] = read(l, s, n)
        for x in range(B):
            for s, n in pieces(w):
                yhi[pl.ds(off + x * w + s, n), :] = read(x, B - w + s, n)
                ylo[pl.ds(off + x * w + s, n), :] = read(x, s, n)
        off += B * w


def corner_kernel(widths, xlo, xhi, yhi, ylo):
    off = o = 0
    for h in widths:
        for slab, layer in ((xlo, lambda a: h - a), (xhi, lambda a: a - 1)):
            for a in range(1, h):
                n = h - a
                base = off + layer(a) * B
                yhi[pl.ds(o, n), :] = slab[pl.ds(base + B - n, n), :]
                ylo[pl.ds(o, n), :] = slab[pl.ds(base, n), :]
                o += n
        off += B * h


def unpack(own, slabs, corners, widths, edges, stores):
    xlo, xhi, ylo, yhi = slabs
    clo, chi = corners
    exlo, exhi, eylo, eyhi = edges
    off = o = 0
    for f, h in enumerate(widths):
        put = stores[f]
        for x in range(B):
            for s, n in pieces(B):
                put(x, s, own[f](x, s, n), None)
        for l in range(h):
            for s, n in pieces(B):
                put(l - h, s, xlo[pl.ds(off + l * B + s, n), :], exlo)
                put(B + l, s, xhi[pl.ds(off + l * B + s, n), :], exhi)
        for x in range(B):
            for s, n in pieces(h):
                put(x, s - h, ylo[pl.ds(off + x * h + s, n), :], eylo)
                put(x, B + s, yhi[pl.ds(off + x * h + s, n), :], eyhi)
        for side, edge in ((0, exlo), (1, exhi)):
            for a in range(1, h):
                n = h - a
                x = -a if side == 0 else B + a - 1
                put(x, -n, clo[pl.ds(o, n), :], jnp.logical_or(edge, eylo))
                put(x, B, chi[pl.ds(o, n), :], jnp.logical_or(edge, eyhi))
                o += n
        off += B * h


def edges_of(place):
    gx, gy = place[0], place[1]
    return gx == 0, gx == place[2] - 1, gy == 0, gy == place[3] - 1


def first_pack_kernel(own, *outs):
    pack_slabs(own_readers(own), mask_widths(), outs)


def own_readers(own):
    return [lambda x, y, n, f=f: own[f, x, pl.ds(y, n), :] for f in range(4)]


def row(x, y):
    return (x + HALO) * YP + y + HALO


def first_kernel(
    sides, place, vector, own, xlo, xhi, ylo, yhi, clo, chi,
    state, fix, ld, cr, own_free, *tough_outs,
):
    w = [vector[i] for i in range(3)]
    edges = edges_of(place)

    def choose(outside, value, other):
        return value if outside is None else jnp.where(outside, other, value)

    def put_fixed(x, y, v, outside):
        fix[pl.ds(row(x, y), v.shape[0]), :] = choose(outside, v, 1.0)
        if outside is None:
            own_free[pl.ds(row(x, y), v.shape[0]), :] = 1.0 - v

    def put_load(x, y, v, outside):
        v = choose(outside, v, 0.0)
        at = pl.ds(row(x, y), v.shape[0])
        ld[at, :] = v
        above, below = up(v), down(v)
        for i in range(3):
            state[i, at, :] = v * w[i]
            state[4 + i, at, :] = above * w[i]
            state[7 + i, at, :] = below * w[i]

    def put_crack(x, y, v, outside):
        at = pl.ds(row(x, y), v.shape[0])
        cr[at, :] = choose(outside, v, -1.0)
        put_state(state, 3, at, choose(outside, v, 0.0))

    def put_tough(x, y, v, outside):
        n = v.shape[0]
        for ref, h in zip(tough_outs, sides):
            lo, hi = max(y, -h), min(y + n, B + h)
            if -h <= x < B + h and lo < hi:
                at = (x + h) * (B + 2 * h) + lo + h
                ref[pl.ds(at, hi - lo), :] = v[lo - y : hi - y]

    own_free[...] = jnp.zeros_like(own_free)
    unpack(
        own_readers(own), (xlo, xhi, ylo, yhi), (clo, chi), mask_widths(), edges,
        (put_fixed, put_load, put_crack, put_tough),
    )


def horner(coefs, w):
    acc = w * coefs[-1] + coefs[-2]
    for c in coefs[-3::-1]:
        acc = acc * w + c
    return acc


def up(v, outside=0.0):
    lane = lax.broadcasted_iota(jnp.int32, v.shape, 1)
    return jnp.where(lane == 127, outside, pltpu.roll(v, 127, 1))


def down(v, outside=0.0):
    lane = lax.broadcasted_iota(jnp.int32, v.shape, 1)
    return jnp.where(lane == 0, outside, pltpu.roll(v, 1, 1))


def put_state(ref, f, at, v):
    ref[f, at, :] = v
    plus, minus = ((4 + f, 7 + f) if f < 3 else (10, 11))
    ref[plus, at, :] = up(v)
    ref[minus, at, :] = down(v)


def sweep(src, dst, half, flow, flow_z, fix, ld, cr, own_free, tough, w, left):
    hd = 2 * left
    hm = hd + 1

    def chunks(h, i):
        base = i * YP + HALO - h
        return [base + 8 * t for t in range(-(-(B + 2 * h) // 8))]

    def flow_row(i):
        for r in chunks(hd + 2, i):
            at = pl.ds(r, 8)
            keep = 1.0 - src[3, at, :]
            h = keep * keep * 0.5 + 0.0005
            div = (
                (src[0, pl.ds(r + YP, 8), :] - src[0, pl.ds(r - YP, 8), :])
                + (src[1, pl.ds(r + 1, 8), :] - src[1, pl.ds(r - 1, 8), :])
                + (src[6, at, :] - src[9, at, :])
            )
            half[at, :] = h
            flow[at, :] = jnp.where(cr[at, :] < -0.5, 0.0, h * div)

    def turned_flow(i):
        out = []
        for r in chunks(hm, i):
            at = pl.ds(r, 8)
            v = flow[at, :]
            out.append((at, up(v) - down(v)))
        return out

    def put_flow_z(done):
        for at, v in done:
            flow_z[at, :] = v

    def turned(ref, fields, h, i):
        out = []
        for r in chunks(h, i):
            at = pl.ds(r, 8)
            for f in fields:
                v = ref[f, at, :]
                plus, minus = ((4 + f, 7 + f) if f < 3 else (10, 11))
                out.append((plus, at, up(v)))
                out.append((minus, at, down(v)))
        return out

    def put_turned(ref, done):
        for f, at, v in done:
            ref[f, at, :] = v

    def half_of(d):
        keep = 1.0 - d
        return keep * keep * 0.5 + 0.0005

    def moved_row(i, acc):
        for r in chunks(hd + 1, i):
            at = pl.ds(r, 8)
            around = [pl.ds(r + d, 8) for d in (YP, -YP, 1, -1)]
            h0 = half[at, :]
            hn = [half[a, :] for a in around] + [half_of(src[10, at, :]), half_of(src[11, at, :])]
            pairs = [hn[0] + hn[1], hn[2] + hn[3], hn[4] + hn[5]]
            weight = 6.0 * h0 + (pairs[0] + pairs[1] + pairs[2])
            faces = [h0 + n for n in hn]
            slope = [
                flow[around[0], :] - flow[around[1], :],
                flow[around[2], :] - flow[around[3], :],
                flow_z[at, :],
            ]
            is_fixed = fix[at, :] > 0.5
            load = ld[at, :]
            squares = None
            for c in range(3):
                u0 = src[c, at, :]
                un = [src[c, a, :] for a in around] + [src[4 + c, at, :], src[7 + c, at, :]]
                res = slope[c] - weight * u0
                for f, n in zip(faces, un):
                    res = res + f * n
                relaxed = u0 + (res * 0.6) / (weight + pairs[c])
                dst[c, at, :] = jnp.where(is_fixed, load * w[c], relaxed)
                squares = res * res if squares is None else squares + res * res
            acc = acc + jnp.where(own_free[at, :] > 0.5, squares, 0.0)
        return acc

    def damage_row(i):
        for t, r in enumerate(chunks(hd, i)):
            at = pl.ds(r, 8)
            g = [
                (
                    dst[k, pl.ds(r + YP, 8), :] - dst[k, pl.ds(r - YP, 8), :],
                    dst[k, pl.ds(r + 1, 8), :] - dst[k, pl.ds(r - 1, 8), :],
                    dst[4 + k, at, :] - dst[7 + k, at, :],
                )
                for k in range(3)
            ]
            total = g[0][0] + g[1][1] + g[2][2]
            third = total * (1.0 / 3.0)
            dx, dy, dz = g[0][0] - third, g[1][1] - third, g[2][2] - third
            xy, xz, yz = g[0][1] + g[1][0], g[0][2] + g[2][0], g[1][2] + g[2][1]
            xy2, xz2, yz2 = xy * xy, xz * xz, yz * yz
            spread = (dx * dx + dy * dy + dz * dz) + 0.5 * (xy2 + xz2 + yz2)
            det = dx * dy * dz + 0.25 * (xy * xz * yz - (dx * yz2 + dy * xz2 + dz * xy2))
            s6 = spread * (1.0 / 24.0)
            inv = lax.rsqrt(s6 + 1e-08)
            ratio = (det * 0.0625) * (inv * inv * inv)
            radius = s6 * lax.rsqrt(jnp.maximum(s6, 1e-37))
            wq = jnp.maximum(0.5 - 0.5 * jnp.abs(ratio), 0.0)
            cos = horner(COS_THIRD, wq)
            sin = (wq * lax.rsqrt(jnp.maximum(wq, 1e-37))) * horner(SIN_THIRD, wq)
            signed = jnp.where(ratio < 0.0, -radius, radius)
            a, b = signed * cos, signed * sin
            mean = total * (1.0 / 6.0)
            l1, rest = mean + 2.0 * a, mean - a
            p1 = jnp.maximum(l1, 0.0)
            p2 = jnp.maximum(rest + b, 0.0)
            p3 = jnp.maximum(rest - b, 0.0)
            trace = jnp.maximum(total, 0.0)
            psi2 = 0.25 * (trace * trace) + 2.0 * (p1 * p1 + p2 * p2 + p3 * p3)
            beside = (
                (src[3, pl.ds(r + YP, 8), :] + src[3, pl.ds(r - YP, 8), :])
                + (src[3, pl.ds(r + 1, 8), :] + src[3, pl.ds(r - 1, 8), :])
                + (src[10, at, :] + src[11, at, :])
            )
            gc = tough[pl.ds((i - (HALO - hd)) * (B + 2 * hd) + 8 * t, 8), :]
            new = (psi2 + gc * beside) / (psi2 + 7.0 * gc)
            kind = cr[at, :]
            dst[3, at, :] = jnp.where(kind > 0.5, 1.0, jnp.where(kind < -0.5, 0.0, new))

    def step(i, acc, damaged):
        later = turned(dst, range(3), hd, i - 1)
        if damaged and left:
            later += turned(dst, (3,), hd - 1, i - 3)
        z_later = turned_flow(i + 1)
        flow_row(i + 2)
        acc = moved_row(i, acc)
        if damaged:
            damage_row(i - 2)
        put_turned(dst, later)
        put_flow_z(z_later)
        return acc

    low, high = HALO - hm, HALO + B + hm
    for i in (low - 1, low, low + 1):
        flow_row(i)
    put_flow_z(turned_flow(low))
    acc = lax.fori_loop(
        low, low + 3, lambda i, c: step(i, c, False), jnp.zeros((8, 128), f32)
    )
    acc = lax.fori_loop(low + 3, high, lambda i, c: step(i, c, True), acc)
    later = turned(dst, (3,), hd - 1, high - 3) if left else ()
    damage_row(high - 2)
    put_turned(dst, later)
    return acc


def add_sum(sums, acc, r):
    lane = lax.broadcasted_iota(jnp.int32, (1, 128), 1)
    return jnp.where(lane % ROUNDS == r, jnp.sum(acc), sums)


def sweep_kernel(segment, *refs):
    group, begin, end = segment
    k = GROUPS[group]
    final = group == len(GROUPS) - 1 and end == k
    refs = list(refs)

    def take(n):
        out = refs[:n]
        del refs[:n]
        return out

    place, vector, fix, ld, cr, own_free, sums_in = take(7)
    tough = take(end - begin)
    w = [vector[i] for i in range(3)]
    unpacks = group > 0 and begin == 0
    if unpacks:
        state, xlo, xhi, ylo, yhi, clo, chi = take(7)
    else:
        (src,) = take(1)
    if final:
        moved_out, damage_out = take(2)
    elif end == k:
        (state_out,) = take(1)
        slab_outs = take(4)
    else:
        (wide_out,) = take(1)
    (sums_out,) = take(1)
    half, flow, flow_z, *bufs = refs
    if unpacks:
        src = bufs[1]

        def own(f):
            return lambda x, y, n: state[f, x, pl.ds(y, n), :]

        def put(f):
            def one(x, y, v, outside):
                v = v if outside is None else jnp.where(outside, 0.0, v)
                put_state(src, f, pl.ds(row(x, y), v.shape[0]), v)

            return one

        unpack(
            [own(f) for f in range(4)], (xlo, xhi, ylo, yhi), (clo, chi), state_widths(k),
            edges_of(place), [put(f) for f in range(4)],
        )
    sums = sums_in[...]
    start = sum(GROUPS[:group])
    for j in range(begin, end):
        dst = wide_out if j == end - 1 and end < k else bufs[j % 2]
        acc = sweep(
            src, dst, half, flow, flow_z, fix, ld, cr, own_free, tough[j - begin], w, k - 1 - j
        )
        sums = add_sum(sums, acc, start + j)
        src = dst
    if final:
        for x in range(B):
            for s, n in pieces(B):
                at = pl.ds(row(x, s), n)
                for c in range(3):
                    moved_out[0, c, x, pl.ds(s, n), :] = src[c, at, :]
                damage_out[0, x, pl.ds(s, n), :] = src[3, at, :]
    elif end == k:
        for f in range(4):
            for x in range(B):
                for s, n in pieces(B):
                    state_out[f, x, pl.ds(s, n), :] = src[f, pl.ds(row(x, s), n), :]
        readers = [(lambda x, y, n, f=f: src[f, pl.ds(row(x, y), n), :]) for f in range(4)]
        pack_slabs(readers, state_widths(GROUPS[group + 1]), slab_outs)
    sums_out[...] = jnp.broadcast_to(sums, sums_out.shape)


def table_kernel(scale, place, parts, out):
    total = jnp.sum(parts[...], axis=0, keepdims=True)
    root = jnp.sqrt(total * scale)
    out[...] = pltpu.roll(jnp.broadcast_to(root, (8, 128)), place[4], 1)[:1, :ROUNDS]


def call(kernel, outs, ins, scratch=(), smem=0, us=1.0, limit=4):
    single = isinstance(outs, tuple)
    shapes = [outs] if single else outs
    shapes = [s if isinstance(s, jax.ShapeDtypeStruct) else jax.ShapeDtypeStruct(s, f32) for s in shapes]
    res = pl.pallas_call(
        kernel,
        out_shape=shapes,
        in_specs=[SMEM] * smem + [VMEM] * (len(ins) - smem),
        out_specs=[VMEM] * len(shapes),
        scratch_shapes=list(scratch),
        compiler_params=pltpu.CompilerParams(vmem_limit_bytes=limit * 1024 * 1024),
        cost_estimate=pl.CostEstimate(
            flops=int(us * 1e9), bytes_accessed=int(us * 1e6), transcendentals=0
        ),
    )(*ins)
    return res[0] if single else res


def shift(x, axis, by):
    n = lax.axis_size(axis)
    return lax.ppermute(x, axis, [(i, (i + by) % n) for i in range(n)])


def swap_sides(slabs):
    xhi, xlo, yhi, ylo = slabs
    return shift(xhi, "gx", 1), shift(xlo, "gx", -1), shift(yhi, "gy", 1), shift(ylo, "gy", -1)


def swap_corners(xlo, xhi, widths):
    shape = (corner_rows(widths), 128)
    yhi, ylo = call(functools.partial(corner_kernel, widths), [shape] * 2, [xlo, xhi], us=0.3)
    return shift(yhi, "gy", 1), shift(ylo, "gy", -1)


def on_device(load_index, load_table, toughness, clamp_mask, load_mask, crack_mask):
    home = lax.axis_index("section").astype(jnp.int32)
    nx, ny = lax.axis_size("gx"), lax.axis_size("gy")
    place = jnp.stack(
        [
            lax.axis_index("gx").astype(jnp.int32),
            lax.axis_index("gy").astype(jnp.int32),
            jnp.int32(nx),
            jnp.int32(ny),
            home,
        ]
    )
    vector = lax.dynamic_slice(load_table, (load_index[0], 0), (1, 3)).reshape(3)
    own = jnp.stack(
        [
            jnp.maximum(clamp_mask, load_mask).astype(f32),
            load_mask.astype(f32),
            crack_mask.astype(f32),
            toughness[0],
        ]
    )
    own = lax.optimization_barrier(own)
    widths = mask_widths()
    slabs = call(first_pack_kernel, [(slab_rows(widths), 128)] * 4, [own], us=0.5)
    received = swap_sides(slabs)
    corners = swap_corners(received[0], received[1], widths)
    sides = tuple(sorted({h for h in T_HALO if h}, reverse=True))
    ext = (ROWS, 128)
    made = call(
        functools.partial(first_kernel, sides),
        [(12,) + ext, ext, ext, ext, ext] + [(rows_of(h), 128) for h in sides],
        [place, vector, own, *received, *corners], smem=2, us=1.9,
    )
    state, kinds = made[0], made[1:5]
    by_halo = dict(zip(sides, made[5:]))
    by_halo[0] = toughness.reshape(B * B, 128)
    tough = []
    for r, h in enumerate(T_HALO):
        tough.append(by_halo[h] if r == 0 else shift(by_halo[h], "section", -r))
    sums = jnp.zeros((1, 128), f32)
    for segment in SEGMENTS:
        g, begin, end = segment
        k = GROUPS[g]
        start = sum(GROUPS[:g])
        ins = [place, vector, *kinds, sums, *tough[start + begin : start + end]]
        unpacks = g > 0 and begin == 0
        if unpacks:
            received = swap_sides(slabs)
            corners = swap_corners(received[0], received[1], state_widths(k))
            ins += [state, *received, *corners]
        else:
            ins.append(state)
        final = g == len(GROUPS) - 1 and end == k
        if final:
            outs = [(1, 3, B, B, 128), (1, B, B, 128), (nx * ny, 128)]
        elif end == k:
            n = slab_rows(state_widths(GROUPS[g + 1]))
            outs = [(4, B, B, 128)] + [(n, 128)] * 4 + [(1, 128)]
        else:
            outs = [(12,) + ext, (1, 128)]
        bufs = 2 if end - begin > 1 else 0
        scratch = [pltpu.VMEM(ext, f32)] * 3 + [pltpu.VMEM((12,) + ext, f32)] * bufs
        cost = sum((B + 4 * (k - 1 - j)) ** 2 * 0.007 for j in range(begin, end))
        res = call(
            functools.partial(sweep_kernel, segment), outs, ins, scratch,
            smem=2, us=cost, limit=4 + 8 * bufs,
        )
        if final:
            moved, damage, parts = res
        elif end == k:
            state, slabs, sums = res[0], res[1:5], res[5]
        else:
            state, sums = res
    parts = lax.all_to_all(parts, ("gx", "gy"), 0, 0, tiled=True)
    scale = 1.0 / (3.0 * B * B * 128 * nx * ny)
    norms = call(
        functools.partial(table_kernel, scale), (1, ROUNDS), [place, parts], smem=1, us=0.1
    )
    return moved, damage, norms


def solution(mesh):
    in_specs = (
        P("section"),
        P(),
        P("section", "gx", "gy", None),
        P("gx", "gy", None),
        P("gx", "gy", None),
        P("gx", "gy", None),
    )
    out_specs = (
        P("section", None, "gx", "gy", None),
        P("section", "gx", "gy", None),
        P("section", None),
    )
    return jax.shard_map(
        on_device, mesh=mesh, in_specs=in_specs, out_specs=out_specs, check_vma=False
    )
```

```python
import functools

import jax
import jax.numpy as jnp
from jax import lax
from jax.experimental import pallas as pl
from jax.experimental.pallas import tpu as pltpu
from jax.sharding import PartitionSpec as P


GROUPS = (4, 4)
B = 16
HALO = 2 * max(GROUPS) + 1
YP = B + 2 * HALO
ROWS = -(-(YP * (YP + 1) + 32) // 8) * 8

COS_THIRD = (
    1.000000008260009, -0.22222426779181312, -0.06576120509434145, -0.035390736331322045,
    -0.012547845736683551, -0.050373368401680454, 0.05848138776830297, -0.07087101496233855,
)
SIN_THIRD = (
    1.1547005306829978, 0.1069186220087089, 0.04565984619644209, 0.027903402002033718,
    0.00953945386696008, 0.04580735112208377, -0.054824704413705544, 0.06541734748383539,
)

ROUNDS = sum(GROUPS)
SEGMENTS = ((0, 0, 1), (0, 1, 2), (0, 2, 4), (1, 0, 4))
PLACES = [(g, j) for g, k in enumerate(GROUPS) for j in range(k)]
T_HALO = [2 * (GROUPS[g] - 1 - j) for g, j in PLACES]
T_MAX = max(T_HALO)
VMEM = pl.BlockSpec(memory_space=pltpu.VMEM)
SMEM = pl.BlockSpec(memory_space=pltpu.SMEM)
f32 = jnp.float32


def rows_of(h):
    side = B + 2 * h
    return side * side if h == 0 else -(-(side * side + 8) // 8) * 8


def mask_widths():
    k = GROUPS[0]
    return (2 * k + 1, 2 * k - 1, 2 * k, T_MAX)


def state_widths(k):
    return (2 * k + 1,) * 3 + (2 * k,)


def tri(h):
    return h * (h - 1) // 2


def slab_rows(widths):
    return B * sum(widths)


def corner_rows(widths):
    return -(-sum(2 * tri(h) for h in widths) // 8) * 8


def pieces(n):
    return [(s, min(8, n - s)) for s in range(0, n, 8)]


def pack_slabs(readers, widths, outs):
    xhi, xlo, yhi, ylo = outs
    off = 0
    for read, w in zip(readers, widths):
        for l in range(w):
            for s, n in pieces(B):
                xhi[pl.ds(off + l * B + s, n), :] = read(B - w + l, s, n)
                xlo[pl.ds(off + l * B + s, n), :] = read(l, s, n)
        for x in range(B):
            for s, n in pieces(w):
                yhi[pl.ds(off + x * w + s, n), :] = read(x, B - w + s, n)
                ylo[pl.ds(off + x * w + s, n), :] = read(x, s, n)
        off += B * w


def corner_kernel(widths, xlo, xhi, yhi, ylo):
    off = o = 0
    for h in widths:
        for slab, layer in ((xlo, lambda a: h - a), (xhi, lambda a: a - 1)):
            for a in range(1, h):
                n = h - a
                base = off + layer(a) * B
                yhi[pl.ds(o, n), :] = slab[pl.ds(base + B - n, n), :]
                ylo[pl.ds(o, n), :] = slab[pl.ds(base, n), :]
                o += n
        off += B * h


def unpack(own, slabs, corners, widths, edges, stores):
    xlo, xhi, ylo, yhi = slabs
    clo, chi = corners
    exlo, exhi, eylo, eyhi = edges
    off = o = 0
    for f, h in enumerate(widths):
        put = stores[f]
        for x in range(B):
            for s, n in pieces(B):
                put(x, s, own[f](x, s, n), None)
        for l in range(h):
            for s, n in pieces(B):
                put(l - h, s, xlo[pl.ds(off + l * B + s, n), :], exlo)
                put(B + l, s, xhi[pl.ds(off + l * B + s, n), :], exhi)
        for x in range(B):
            for s, n in pieces(h):
                put(x, s - h, ylo[pl.ds(off + x * h + s, n), :], eylo)
                put(x, B + s, yhi[pl.ds(off + x * h + s, n), :], eyhi)
        for side, edge in ((0, exlo), (1, exhi)):
            for a in range(1, h):
                n = h - a
                x = -a if side == 0 else B + a - 1
                put(x, -n, clo[pl.ds(o, n), :], jnp.logical_or(edge, eylo))
                put(x, B, chi[pl.ds(o, n), :], jnp.logical_or(edge, eyhi))
                o += n
        off += B * h


def edges_of(place):
    gx, gy = place[0], place[1]
    return gx == 0, gx == place[2] - 1, gy == 0, gy == place[3] - 1


def first_pack_kernel(masks, tough, *outs):
    pack_slabs(own_readers(masks, tough), mask_widths(), outs)


def own_readers(masks, tough):
    readers = [lambda x, y, n, f=f: masks[f, x, pl.ds(y, n), :].astype(f32) for f in range(3)]
    return readers + [lambda x, y, n: tough[0, x, pl.ds(y, n), :]]


def row(x, y):
    return (x + HALO) * YP + y + HALO


def first_kernel(
    sides, place, vector, masks, own_tough, xlo, xhi, ylo, yhi, clo, chi,
    state, fix, ld, cr, own_free, *tough_outs,
):
    w = [vector[i] for i in range(3)]
    edges = edges_of(place)

    def choose(outside, value, other):
        return value if outside is None else jnp.where(outside, other, value)

    def put_clamp(x, y, v, outside):
        at = pl.ds(row(x, y), v.shape[0])
        v = jnp.maximum(choose(outside, v, 1.0), ld[at, :])
        fix[at, :] = v
        if outside is None:
            own_free[at, :] = 1.0 - v

    def put_load(x, y, v, outside):
        v = choose(outside, v, 0.0)
        at = pl.ds(row(x, y), v.shape[0])
        ld[at, :] = v
        above, below = up(v), down(v)
        for i in range(3):
            state[i, at, :] = v * w[i]
            state[4 + i, at, :] = above * w[i]
            state[7 + i, at, :] = below * w[i]

    def put_crack(x, y, v, outside):
        at = pl.ds(row(x, y), v.shape[0])
        cr[at, :] = choose(outside, v, -1.0)
        put_state(state, 3, at, choose(outside, v, 0.0))

    def put_tough(x, y, v, outside):
        n = v.shape[0]
        for ref, h in zip(tough_outs, sides):
            lo, hi = max(y, -h), min(y + n, B + h)
            if -h <= x < B + h and lo < hi:
                at = (x + h) * (B + 2 * h) + lo + h
                ref[pl.ds(at, hi - lo), :] = v[lo - y : hi - y]

    own_free[...] = jnp.zeros_like(own_free)
    unpack(
        own_readers(masks, own_tough), (xlo, xhi, ylo, yhi), (clo, chi), mask_widths(), edges,
        (put_load, put_clamp, put_crack, put_tough),
    )


def horner(coefs, w):
    acc = w * coefs[-1] + coefs[-2]
    for c in coefs[-3::-1]:
        acc = acc * w + c
    return acc


def up(v, outside=0.0):
    lane = lax.broadcasted_iota(jnp.int32, v.shape, 1)
    return jnp.where(lane == 127, outside, pltpu.roll(v, 127, 1))


def down(v, outside=0.0):
    lane = lax.broadcasted_iota(jnp.int32, v.shape, 1)
    return jnp.where(lane == 0, outside, pltpu.roll(v, 1, 1))


def put_state(ref, f, at, v):
    ref[f, at, :] = v
    plus, minus = ((4 + f, 7 + f) if f < 3 else (10, 11))
    ref[plus, at, :] = up(v)
    ref[minus, at, :] = down(v)


def sweep(src, dst, half, flow, flow_z, fix, ld, cr, own_free, tough, w, left):
    hd = 2 * left
    hm = hd + 1

    def chunks(h, i):
        base = i * YP + HALO - h
        return [base + 8 * t for t in range(-(-(B + 2 * h) // 8))]

    def flow_row(i):
        for r in chunks(hd + 2, i):
            at = pl.ds(r, 8)
            keep = 1.0 - src[3, at, :]
            h = keep * keep * 0.5 + 0.0005
            div = (
                (src[0, pl.ds(r + YP, 8), :] - src[0, pl.ds(r - YP, 8), :])
                + (src[1, pl.ds(r + 1, 8), :] - src[1, pl.ds(r - 1, 8), :])
                + (src[6, at, :] - src[9, at, :])
            )
            half[at, :] = h
            flow[at, :] = jnp.where(cr[at, :] < -0.5, 0.0, h * div)

    def turned_flow(i):
        out = []
        for r in chunks(hm, i):
            at = pl.ds(r, 8)
            v = flow[at, :]
            out.append((at, up(v) - down(v)))
        return out

    def put_flow_z(done):
        for at, v in done:
            flow_z[at, :] = v

    def turned(ref, fields, h, i):
        out = []
        for r in chunks(h, i):
            at = pl.ds(r, 8)
            for f in fields:
                v = ref[f, at, :]
                plus, minus = ((4 + f, 7 + f) if f < 3 else (10, 11))
                out.append((plus, at, up(v)))
                out.append((minus, at, down(v)))
        return out

    def put_turned(ref, done):
        for f, at, v in done:
            ref[f, at, :] = v

    def half_of(d):
        keep = 1.0 - d
        return keep * keep * 0.5 + 0.0005

    def moved_row(i, acc):
        for r in chunks(hd + 1, i):
            at = pl.ds(r, 8)
            around = [pl.ds(r + d, 8) for d in (YP, -YP, 1, -1)]
            h0 = half[at, :]
            hn = [half[a, :] for a in around] + [half_of(src[10, at, :]), half_of(src[11, at, :])]
            pairs = [hn[0] + hn[1], hn[2] + hn[3], hn[4] + hn[5]]
            weight = 6.0 * h0 + (pairs[0] + pairs[1] + pairs[2])
            faces = [h0 + n for n in hn]
            slope = [
                flow[around[0], :] - flow[around[1], :],
                flow[around[2], :] - flow[around[3], :],
                flow_z[at, :],
            ]
            is_fixed = fix[at, :] > 0.5
            load = ld[at, :]
            squares = None
            for c in range(3):
                u0 = src[c, at, :]
                un = [src[c, a, :] for a in around] + [src[4 + c, at, :], src[7 + c, at, :]]
                res = slope[c] - weight * u0
                for f, n in zip(faces, un):
                    res = res + f * n
                relaxed = u0 + (res * 0.6) / (weight + pairs[c])
                dst[c, at, :] = jnp.where(is_fixed, load * w[c], relaxed)
                squares = res * res if squares is None else squares + res * res
            acc = acc + jnp.where(own_free[at, :] > 0.5, squares, 0.0)
        return acc

    def damage_row(i):
        for t, r in enumerate(chunks(hd, i)):
            at = pl.ds(r, 8)
            g = [
                (
                    dst[k, pl.ds(r + YP, 8), :] - dst[k, pl.ds(r - YP, 8), :],
                    dst[k, pl.ds(r + 1, 8), :] - dst[k, pl.ds(r - 1, 8), :],
                    dst[4 + k, at, :] - dst[7 + k, at, :],
                )
                for k in range(3)
            ]
            total = g[0][0] + g[1][1] + g[2][2]
            third = total * (1.0 / 3.0)
            dx, dy, dz = g[0][0] - third, g[1][1] - third, g[2][2] - third
            xy, xz, yz = g[0][1] + g[1][0], g[0][2] + g[2][0], g[1][2] + g[2][1]
            xy2, xz2, yz2 = xy * xy, xz * xz, yz * yz
            spread = (dx * dx + dy * dy + dz * dz) + 0.5 * (xy2 + xz2 + yz2)
            det = dx * dy * dz + 0.25 * (xy * xz * yz - (dx * yz2 + dy * xz2 + dz * xy2))
            s6 = spread * (1.0 / 24.0)
            inv = lax.rsqrt(s6 + 1e-08)
            ratio = (det * 0.0625) * (inv * inv * inv)
            radius = s6 * lax.rsqrt(jnp.maximum(s6, 1e-37))
            wq = jnp.maximum(0.5 - 0.5 * jnp.abs(ratio), 0.0)
            cos = horner(COS_THIRD, wq)
            sin = (wq * lax.rsqrt(jnp.maximum(wq, 1e-37))) * horner(SIN_THIRD, wq)
            signed = jnp.where(ratio < 0.0, -radius, radius)
            a, b = signed * cos, signed * sin
            mean = total * (1.0 / 6.0)
            l1, rest = mean + 2.0 * a, mean - a
            p1 = jnp.maximum(l1, 0.0)
            p2 = jnp.maximum(rest + b, 0.0)
            p3 = jnp.maximum(rest - b, 0.0)
            trace = jnp.maximum(total, 0.0)
            psi2 = 0.25 * (trace * trace) + 2.0 * (p1 * p1 + p2 * p2 + p3 * p3)
            beside = (
                (src[3, pl.ds(r + YP, 8), :] + src[3, pl.ds(r - YP, 8), :])
                + (src[3, pl.ds(r + 1, 8), :] + src[3, pl.ds(r - 1, 8), :])
                + (src[10, at, :] + src[11, at, :])
            )
            gc = tough[pl.ds((i - (HALO - hd)) * (B + 2 * hd) + 8 * t, 8), :]
            new = (psi2 + gc * beside) / (psi2 + 7.0 * gc)
            kind = cr[at, :]
            dst[3, at, :] = jnp.where(kind > 0.5, 1.0, jnp.where(kind < -0.5, 0.0, new))

    def step(i, acc, damaged):
        later = turned(dst, range(3), hd, i - 1)
        if damaged and left:
            later += turned(dst, (3,), hd - 1, i - 3)
        z_later = turned_flow(i + 1)
        flow_row(i + 2)
        acc = moved_row(i, acc)
        if damaged:
            damage_row(i - 2)
        put_turned(dst, later)
        put_flow_z(z_later)
        return acc

    low, high = HALO - hm, HALO + B + hm
    for i in (low - 1, low, low + 1):
        flow_row(i)
    put_flow_z(turned_flow(low))
    acc = lax.fori_loop(
        low, low + 3, lambda i, c: step(i, c, False), jnp.zeros((8, 128), f32)
    )
    acc = lax.fori_loop(low + 3, high, lambda i, c: step(i, c, True), acc)
    later = turned(dst, (3,), hd - 1, high - 3) if left else ()
    damage_row(high - 2)
    put_turned(dst, later)
    return acc


def add_sum(sums, acc, r):
    lane = lax.broadcasted_iota(jnp.int32, (1, 128), 1)
    return jnp.where(lane % ROUNDS == r, jnp.sum(acc), sums)


def sweep_kernel(segment, *refs):
    group, begin, end = segment
    k = GROUPS[group]
    final = group == len(GROUPS) - 1 and end == k
    refs = list(refs)

    def take(n):
        out = refs[:n]
        del refs[:n]
        return out

    place, vector, fix, ld, cr, own_free, sums_in = take(7)
    tough = take(end - begin)
    w = [vector[i] for i in range(3)]
    unpacks = group > 0 and begin == 0
    if unpacks:
        state, xlo, xhi, ylo, yhi, clo, chi = take(7)
    else:
        (src,) = take(1)
    if final:
        moved_out, damage_out = take(2)
    elif end == k:
        (state_out,) = take(1)
        slab_outs = take(4)
    else:
        (wide_out,) = take(1)
    (sums_out,) = take(1)
    half, flow, flow_z, *bufs = refs
    if unpacks:
        src = bufs[1]

        def own(f):
            return lambda x, y, n: state[f, x, pl.ds(y, n), :]

        def put(f):
            def one(x, y, v, outside):
                v = v if outside is None else jnp.where(outside, 0.0, v)
                put_state(src, f, pl.ds(row(x, y), v.shape[0]), v)

            return one

        unpack(
            [own(f) for f in range(4)], (xlo, xhi, ylo, yhi), (clo, chi), state_widths(k),
            edges_of(place), [put(f) for f in range(4)],
        )
    sums = sums_in[...]
    start = sum(GROUPS[:group])
    for j in range(begin, end):
        dst = wide_out if j == end - 1 and end < k else bufs[j % 2]
        acc = sweep(
            src, dst, half, flow, flow_z, fix, ld, cr, own_free, tough[j - begin], w, k - 1 - j
        )
        sums = add_sum(sums, acc, start + j)
        src = dst
    if final:
        for x in range(B):
            for s, n in pieces(B):
                at = pl.ds(row(x, s), n)
                for c in range(3):
                    moved_out[0, c, x, pl.ds(s, n), :] = src[c, at, :]
                damage_out[0, x, pl.ds(s, n), :] = src[3, at, :]
    elif end == k:
        for f in range(4):
            for x in range(B):
                for s, n in pieces(B):
                    state_out[f, x, pl.ds(s, n), :] = src[f, pl.ds(row(x, s), n), :]
        readers = [(lambda x, y, n, f=f: src[f, pl.ds(row(x, y), n), :]) for f in range(4)]
        pack_slabs(readers, state_widths(GROUPS[group + 1]), slab_outs)
    sums_out[...] = jnp.broadcast_to(sums, sums_out.shape)


def call(kernel, outs, ins, scratch=(), smem=0, us=1.0, limit=4):
    single = isinstance(outs, tuple)
    shapes = [outs] if single else outs
    shapes = [s if isinstance(s, jax.ShapeDtypeStruct) else jax.ShapeDtypeStruct(s, f32) for s in shapes]
    res = pl.pallas_call(
        kernel,
        out_shape=shapes,
        in_specs=[SMEM] * smem + [VMEM] * (len(ins) - smem),
        out_specs=[VMEM] * len(shapes),
        scratch_shapes=list(scratch),
        compiler_params=pltpu.CompilerParams(vmem_limit_bytes=limit * 1024 * 1024),
        cost_estimate=pl.CostEstimate(
            flops=int(us * 1e9), bytes_accessed=int(us * 1e6), transcendentals=0
        ),
    )(*ins)
    return res[0] if single else res


def shift(x, axis, by):
    n = lax.axis_size(axis)
    return lax.ppermute(x, axis, [(i, (i + by) % n) for i in range(n)])


def swap_sides(slabs):
    xhi, xlo, yhi, ylo = slabs
    return shift(xhi, "gx", 1), shift(xlo, "gx", -1), shift(yhi, "gy", 1), shift(ylo, "gy", -1)


def swap_corners(xlo, xhi, widths):
    shape = (corner_rows(widths), 128)
    yhi, ylo = call(functools.partial(corner_kernel, widths), [shape] * 2, [xlo, xhi], us=0.3)
    return shift(yhi, "gy", 1), shift(ylo, "gy", -1)


def on_device(load_index, load_table, toughness, clamp_mask, load_mask, crack_mask):
    home = lax.axis_index("section").astype(jnp.int32)
    nx, ny = lax.axis_size("gx"), lax.axis_size("gy")
    place = jnp.stack(
        [
            lax.axis_index("gx").astype(jnp.int32),
            lax.axis_index("gy").astype(jnp.int32),
            jnp.int32(nx),
            jnp.int32(ny),
        ]
    )
    vector = lax.dynamic_slice(load_table, (load_index[0], 0), (1, 3)).reshape(3)
    masks = lax.optimization_barrier(jnp.stack([load_mask, clamp_mask, crack_mask]))
    widths = mask_widths()
    slabs = call(first_pack_kernel, [(slab_rows(widths), 128)] * 4, [masks, toughness], us=0.5)
    received = swap_sides(slabs)
    corners = swap_corners(received[0], received[1], widths)
    sides = tuple(sorted({h for h in T_HALO if h}, reverse=True))
    ext = (ROWS, 128)
    made = call(
        functools.partial(first_kernel, sides),
        [(12,) + ext, ext, ext, ext, ext] + [(rows_of(h), 128) for h in sides],
        [place, vector, masks, toughness, *received, *corners], smem=2, us=1.9,
    )
    state, kinds = made[0], made[1:5]
    by_halo = dict(zip(sides, made[5:]))
    by_halo[0] = toughness.reshape(B * B, 128)
    tough = []
    for r, h in enumerate(T_HALO):
        tough.append(by_halo[h] if r == 0 else shift(by_halo[h], "section", -r))
    sums = jnp.zeros((1, 128), f32)
    for segment in SEGMENTS:
        g, begin, end = segment
        k = GROUPS[g]
        start = sum(GROUPS[:g])
        ins = [place, vector, *kinds, sums, *tough[start + begin : start + end]]
        unpacks = g > 0 and begin == 0
        if unpacks:
            received = swap_sides(slabs)
            corners = swap_corners(received[0], received[1], state_widths(k))
            ins += [state, *received, *corners]
        else:
            ins.append(state)
        final = g == len(GROUPS) - 1 and end == k
        if final:
            outs = [(1, 3, B, B, 128), (1, B, B, 128), (nx * ny, 128)]
        elif end == k:
            n = slab_rows(state_widths(GROUPS[g + 1]))
            outs = [(4, B, B, 128)] + [(n, 128)] * 4 + [(1, 128)]
        else:
            outs = [(12,) + ext, (1, 128)]
        bufs = 2 if end - begin > 1 else 0
        scratch = [pltpu.VMEM(ext, f32)] * 3 + [pltpu.VMEM((12,) + ext, f32)] * bufs
        cost = sum((B + 4 * (k - 1 - j)) ** 2 * 0.007 for j in range(begin, end))
        res = call(
            functools.partial(sweep_kernel, segment), outs, ins, scratch,
            smem=2, us=cost, limit=4 + 8 * bufs,
        )
        if final:
            moved, damage, parts = res
        elif end == k:
            state, slabs, sums = res[0], res[1:5], res[5]
        else:
            state, sums = res
    parts = lax.all_to_all(parts, ("gx", "gy"), 0, 0, tiled=True)
    scale = 1.0 / (3.0 * B * B * 128 * nx * ny)
    parts = lax.dynamic_slice(parts, (0, ROUNDS - home), (nx * ny, ROUNDS))
    norms = jnp.sqrt(jnp.sum(parts, axis=0, keepdims=True) * scale)
    return moved, damage, norms


def solution(mesh):
    in_specs = (
        P("section"),
        P(),
        P("section", "gx", "gy", None),
        P("gx", "gy", None),
        P("gx", "gy", None),
        P("gx", "gy", None),
    )
    out_specs = (
        P("section", None, "gx", "gy", None),
        P("section", "gx", "gy", None),
        P("section", None),
    )
    return jax.shard_map(
        on_device, mesh=mesh, in_specs=in_specs, out_specs=out_specs, check_vma=False
    )
```

```python
import functools

import jax
import jax.numpy as jnp
from jax import lax
from jax.experimental import pallas as pl
from jax.experimental.pallas import tpu as pltpu
from jax.sharding import PartitionSpec as P


GROUPS = (4, 4)
B = 16
HALO = 2 * max(GROUPS) + 1
YP = B + 2 * HALO
ROWS = -(-(YP * (YP + 1) + 32) // 8) * 8

COS_THIRD = (
    1.000000008260009, -0.22222426779181312, -0.06576120509434145, -0.035390736331322045,
    -0.012547845736683551, -0.050373368401680454, 0.05848138776830297, -0.07087101496233855,
)
SIN_THIRD = (
    1.1547005306829978, 0.1069186220087089, 0.04565984619644209, 0.027903402002033718,
    0.00953945386696008, 0.04580735112208377, -0.054824704413705544, 0.06541734748383539,
)

SCALE = 16.0 ** (2.0 / 3.0)
ROUNDS = sum(GROUPS)
SEGMENTS = ((0, 0, 1), (0, 1, 2), (0, 2, 4), (1, 0, 4))
PLACES = [(g, j) for g, k in enumerate(GROUPS) for j in range(k)]
T_HALO = [2 * (GROUPS[g] - 1 - j) for g, j in PLACES]
T_MAX = max(T_HALO)
VMEM = pl.BlockSpec(memory_space=pltpu.VMEM)
SMEM = pl.BlockSpec(memory_space=pltpu.SMEM)
f32 = jnp.float32


def rows_of(h):
    side = B + 2 * h
    return side * side if h == 0 else -(-(side * side + 8) // 8) * 8


def mask_widths():
    k = GROUPS[0]
    return (2 * k + 1, 2 * k - 1, 2 * k, T_MAX)


def state_widths(k):
    return (2 * k + 1,) * 3 + (2 * k,)


def tri(h):
    return h * (h - 1) // 2


def slab_rows(widths):
    return B * sum(widths)


def corner_rows(widths):
    return -(-sum(2 * tri(h) for h in widths) // 8) * 8


def pieces(n):
    return [(s, min(8, n - s)) for s in range(0, n, 8)]


def pack_slabs(readers, widths, outs):
    xhi, xlo, yhi, ylo = outs
    off = 0
    for read, w in zip(readers, widths):
        for l in range(w):
            for s, n in pieces(B):
                xhi[pl.ds(off + l * B + s, n), :] = read(B - w + l, s, n)
                xlo[pl.ds(off + l * B + s, n), :] = read(l, s, n)
        for x in range(B):
            for s, n in pieces(w):
                yhi[pl.ds(off + x * w + s, n), :] = read(x, B - w + s, n)
                ylo[pl.ds(off + x * w + s, n), :] = read(x, s, n)
        off += B * w


def corner_kernel(widths, xlo, xhi, yhi, ylo):
    off = o = 0
    for h in widths:
        for slab, layer in ((xlo, lambda a: h - a), (xhi, lambda a: a - 1)):
            for a in range(1, h):
                n = h - a
                base = off + layer(a) * B
                yhi[pl.ds(o, n), :] = slab[pl.ds(base + B - n, n), :]
                ylo[pl.ds(o, n), :] = slab[pl.ds(base, n), :]
                o += n
        off += B * h


def unpack(own, slabs, corners, widths, edges, stores):
    xlo, xhi, ylo, yhi = slabs
    clo, chi = corners
    exlo, exhi, eylo, eyhi = edges
    off = o = 0
    for f, h in enumerate(widths):
        put = stores[f]
        for x in range(B):
            for s, n in pieces(B):
                put(x, s, own[f](x, s, n), None)
        for l in range(h):
            for s, n in pieces(B):
                put(l - h, s, xlo[pl.ds(off + l * B + s, n), :], exlo)
                put(B + l, s, xhi[pl.ds(off + l * B + s, n), :], exhi)
        for x in range(B):
            for s, n in pieces(h):
                put(x, s - h, ylo[pl.ds(off + x * h + s, n), :], eylo)
                put(x, B + s, yhi[pl.ds(off + x * h + s, n), :], eyhi)
        for side, edge in ((0, exlo), (1, exhi)):
            for a in range(1, h):
                n = h - a
                x = -a if side == 0 else B + a - 1
                put(x, -n, clo[pl.ds(o, n), :], jnp.logical_or(edge, eylo))
                put(x, B, chi[pl.ds(o, n), :], jnp.logical_or(edge, eyhi))
                o += n
        off += B * h


def edges_of(place):
    gx, gy = place[0], place[1]
    return gx == 0, gx == place[2] - 1, gy == 0, gy == place[3] - 1


def first_pack_kernel(masks, tough, kept, *outs):
    kept[...] = tough[...]
    pack_slabs(own_readers(masks, tough), mask_widths(), outs)


def own_readers(masks, tough):
    readers = [lambda x, y, n, f=f: masks[f, x, pl.ds(y, n), :].astype(f32) for f in range(3)]
    return readers + [lambda x, y, n: tough[0, x, pl.ds(y, n), :]]


def row(x, y):
    return (x + HALO) * YP + y + HALO


def first_kernel(
    sides, place, vector, masks, own_tough, xlo, xhi, ylo, yhi, clo, chi,
    state, fix, least, most, own_free, *rest,
):
    *tough_outs, ld = rest
    w = [vector[i] for i in range(3)]
    edges = edges_of(place)

    def choose(outside, value, other):
        return value if outside is None else jnp.where(outside, other, value)

    def put_clamp(x, y, v, outside):
        at = pl.ds(row(x, y), v.shape[0])
        v = jnp.maximum(choose(outside, v, 1.0), ld[at, :])
        fix[at, :] = v
        if outside is None:
            own_free[at, :] = 1.0 - v

    def put_load(x, y, v, outside):
        v = choose(outside, v, 0.0)
        at = pl.ds(row(x, y), v.shape[0])
        ld[at, :] = v
        above, below = up(v), down(v)
        for i in range(3):
            state[i, at, :] = v * w[i]
            state[4 + i, at, :] = above * w[i]
            state[7 + i, at, :] = below * w[i]

    def put_crack(x, y, v, outside):
        at = pl.ds(row(x, y), v.shape[0])
        v = choose(outside, v, 0.0)
        least[at, :] = v
        most[at, :] = choose(outside, jnp.ones_like(v), 0.0)
        put_state(state, 3, at, v)

    def put_tough(x, y, v, outside):
        n = v.shape[0]
        for ref, h in zip(tough_outs, sides):
            lo, hi = max(y, -h), min(y + n, B + h)
            if -h <= x < B + h and lo < hi:
                at = (x + h) * (B + 2 * h) + lo + h
                ref[pl.ds(at, hi - lo), :] = v[lo - y : hi - y]

    own_free[...] = jnp.zeros_like(own_free)
    unpack(
        own_readers(masks, own_tough), (xlo, xhi, ylo, yhi), (clo, chi), mask_widths(), edges,
        (put_load, put_clamp, put_crack, put_tough),
    )


def horner(coefs, w):
    acc = w * coefs[-1] + coefs[-2]
    for c in coefs[-3::-1]:
        acc = acc * w + c
    return acc


def up(v, outside=0.0):
    lane = lax.broadcasted_iota(jnp.int32, v.shape, 1)
    return jnp.where(lane == 127, outside, pltpu.roll(v, 127, 1))


def down(v, outside=0.0):
    lane = lax.broadcasted_iota(jnp.int32, v.shape, 1)
    return jnp.where(lane == 0, outside, pltpu.roll(v, 1, 1))


def put_state(ref, f, at, v):
    ref[f, at, :] = v
    plus, minus = ((4 + f, 7 + f) if f < 3 else (10, 11))
    ref[plus, at, :] = up(v)
    ref[minus, at, :] = down(v)


def sweep(src, dst, half, flow, flow_z, given, fix, least, most, own_free, tough, left):
    hd = 2 * left
    hm = hd + 1

    def chunks(h, i):
        base = i * YP + HALO - h
        return [base + 8 * t for t in range(-(-(B + 2 * h) // 8))]

    def flow_row(i):
        for r in chunks(hd + 2, i):
            at = pl.ds(r, 8)
            keep = 1.0 - src[3, at, :]
            h = keep * keep * 0.5 + 0.0005
            div = (
                (src[0, pl.ds(r + YP, 8), :] - src[0, pl.ds(r - YP, 8), :])
                + (src[1, pl.ds(r + 1, 8), :] - src[1, pl.ds(r - 1, 8), :])
                + (src[6, at, :] - src[9, at, :])
            )
            half[at, :] = h
            flow[at, :] = h * div * most[at, :]

    def turned_flow(i):
        out = []
        for r in chunks(hm, i):
            at = pl.ds(r, 8)
            v = flow[at, :]
            out.append((at, up(v) - down(v)))
        return out

    def put_flow_z(done):
        for at, v in done:
            flow_z[at, :] = v

    def turned(ref, fields, h, i):
        out = []
        for r in chunks(h, i):
            at = pl.ds(r, 8)
            for f in fields:
                v = ref[f, at, :]
                plus, minus = ((4 + f, 7 + f) if f < 3 else (10, 11))
                out.append((plus, at, up(v)))
                out.append((minus, at, down(v)))
        return out

    def put_turned(ref, done):
        for f, at, v in done:
            ref[f, at, :] = v

    def half_of(d):
        keep = 1.0 - d
        return keep * keep * 0.5 + 0.0005

    def moved_row(i, acc):
        for r in chunks(hd + 1, i):
            at = pl.ds(r, 8)
            around = [pl.ds(r + d, 8) for d in (YP, -YP, 1, -1)]
            h0 = half[at, :]
            hn = [half[a, :] for a in around] + [half_of(src[10, at, :]), half_of(src[11, at, :])]
            pairs = [hn[0] + hn[1], hn[2] + hn[3], hn[4] + hn[5]]
            weight = 6.0 * h0 + (pairs[0] + pairs[1] + pairs[2])
            faces = [h0 + n for n in hn]
            slope = [
                flow[around[0], :] - flow[around[1], :],
                flow[around[2], :] - flow[around[3], :],
                flow_z[at, :],
            ]
            is_fixed = fix[at, :] > 0.5
            squares = None
            for c in range(3):
                u0 = src[c, at, :]
                un = [src[c, a, :] for a in around] + [src[4 + c, at, :], src[7 + c, at, :]]
                res = slope[c] - weight * u0
                for f, n in zip(faces, un):
                    res = res + f * n
                relaxed = u0 + (res * 0.6) / (weight + pairs[c])
                dst[c, at, :] = jnp.where(is_fixed, given[c, at, :], relaxed)
                squares = res * res if squares is None else squares + res * res
            acc = acc + jnp.where(own_free[at, :] > 0.5, squares, 0.0)
        return acc

    def damage_row(i):
        for t, r in enumerate(chunks(hd, i)):
            at = pl.ds(r, 8)
            g = [
                (
                    dst[k, pl.ds(r + YP, 8), :] - dst[k, pl.ds(r - YP, 8), :],
                    dst[k, pl.ds(r + 1, 8), :] - dst[k, pl.ds(r - 1, 8), :],
                    dst[4 + k, at, :] - dst[7 + k, at, :],
                )
                for k in range(3)
            ]
            total = g[0][0] + g[1][1] + g[2][2]
            third = total * (1.0 / 3.0)
            dx, dy, dz = g[0][0] - third, g[1][1] - third, g[2][2] - third
            xy, xz, yz = g[0][1] + g[1][0], g[0][2] + g[2][0], g[1][2] + g[2][1]
            xy2, xz2, yz2 = xy * xy, xz * xz, yz * yz
            spread = (dx * dx + dy * dy + dz * dz) + 0.5 * (xy2 + xz2 + yz2)
            det = dx * dy * dz + 0.25 * (xy * xz * yz - (dx * yz2 + dy * xz2 + dz * xy2))
            s6 = spread * (1.0 / 24.0)
            inv = lax.rsqrt(spread * (SCALE / 24.0) + 1e-08 * SCALE)
            ratio = det * (inv * inv * inv)
            radius = s6 * lax.rsqrt(jnp.maximum(s6, 1e-37))
            wq = jnp.maximum(0.5 - 0.5 * jnp.abs(ratio), 0.0)
            cos = horner(COS_THIRD, wq)
            sin = (wq * lax.rsqrt(jnp.maximum(wq, 1e-37))) * horner(SIN_THIRD, wq)
            signed = jnp.where(ratio < 0.0, -radius, radius)
            a, b = signed * cos, signed * sin
            mean = total * (1.0 / 6.0)
            l1, rest = mean + 2.0 * a, mean - a
            p1 = jnp.maximum(l1, 0.0)
            p2 = jnp.maximum(rest + b, 0.0)
            p3 = jnp.maximum(rest - b, 0.0)
            trace = jnp.maximum(total, 0.0)
            psi2 = 0.25 * (trace * trace) + 2.0 * (p1 * p1 + p2 * p2 + p3 * p3)
            beside = (
                (src[3, pl.ds(r + YP, 8), :] + src[3, pl.ds(r - YP, 8), :])
                + (src[3, pl.ds(r + 1, 8), :] + src[3, pl.ds(r - 1, 8), :])
                + (src[10, at, :] + src[11, at, :])
            )
            gc = tough[pl.ds((i - (HALO - hd)) * (B + 2 * hd) + 8 * t, 8), :]
            new = (psi2 + gc * beside) / (psi2 + 7.0 * gc)
            dst[3, at, :] = jnp.minimum(jnp.maximum(new, least[at, :]), most[at, :])

    def step(i, acc, damaged):
        later = turned(dst, range(3), hd, i - 1)
        if damaged and left:
            later += turned(dst, (3,), hd - 1, i - 3)
        z_later = turned_flow(i + 1)
        flow_row(i + 2)
        acc = moved_row(i, acc)
        if damaged:
            damage_row(i - 2)
        put_turned(dst, later)
        put_flow_z(z_later)
        return acc

    low, high = HALO - hm, HALO + B + hm
    for i in (low - 1, low, low + 1):
        flow_row(i)
    put_flow_z(turned_flow(low))
    acc = lax.fori_loop(
        low, low + 3, lambda i, c: step(i, c, False), jnp.zeros((8, 128), f32)
    )
    acc = lax.fori_loop(low + 3, high, lambda i, c: step(i, c, True), acc)
    later = turned(dst, (3,), hd - 1, high - 3) if left else ()
    damage_row(high - 2)
    put_turned(dst, later)
    return acc


def add_sum(sums, acc, r):
    lane = lax.broadcasted_iota(jnp.int32, (1, 128), 1)
    return jnp.where(lane % ROUNDS == r, jnp.sum(acc), sums)


def sweep_kernel(segment, *refs):
    group, begin, end = segment
    k = GROUPS[group]
    final = group == len(GROUPS) - 1 and end == k
    refs = list(refs)

    def take(n):
        out = refs[:n]
        del refs[:n]
        return out

    place, given, fix, least, most, own_free, sums_in = take(7)
    tough = take(end - begin)
    unpacks = group > 0 and begin == 0
    if unpacks:
        state, xlo, xhi, ylo, yhi, clo, chi = take(7)
    else:
        (src,) = take(1)
    if final:
        moved_out, damage_out = take(2)
    elif end == k:
        (state_out,) = take(1)
        slab_outs = take(4)
    else:
        (wide_out,) = take(1)
    (sums_out,) = take(1)
    half, flow, flow_z, *bufs = refs
    if unpacks:
        src = bufs[1]

        def own(f):
            return lambda x, y, n: state[f, x, pl.ds(y, n), :]

        def put(f):
            def one(x, y, v, outside):
                v = v if outside is None else jnp.where(outside, 0.0, v)
                put_state(src, f, pl.ds(row(x, y), v.shape[0]), v)

            return one

        unpack(
            [own(f) for f in range(4)], (xlo, xhi, ylo, yhi), (clo, chi), state_widths(k),
            edges_of(place), [put(f) for f in range(4)],
        )
    sums = sums_in[...]
    start = sum(GROUPS[:group])
    for j in range(begin, end):
        dst = wide_out if j == end - 1 and end < k else bufs[j % 2]
        acc = sweep(
            src, dst, half, flow, flow_z, given, fix, least, most, own_free, tough[j - begin],
            k - 1 - j,
        )
        sums = add_sum(sums, acc, start + j)
        src = dst
    if final:
        for x in range(B):
            for s, n in pieces(B):
                at = pl.ds(row(x, s), n)
                for c in range(3):
                    moved_out[0, c, x, pl.ds(s, n), :] = src[c, at, :]
                damage_out[0, x, pl.ds(s, n), :] = src[3, at, :]
    elif end == k:
        for f in range(4):
            for x in range(B):
                for s, n in pieces(B):
                    state_out[f, x, pl.ds(s, n), :] = src[f, pl.ds(row(x, s), n), :]
        readers = [(lambda x, y, n, f=f: src[f, pl.ds(row(x, y), n), :]) for f in range(4)]
        pack_slabs(readers, state_widths(GROUPS[group + 1]), slab_outs)
    sums_out[...] = jnp.broadcast_to(sums, sums_out.shape)


def call(kernel, outs, ins, scratch=(), smem=0, us=1.0, limit=4):
    single = isinstance(outs, tuple)
    shapes = [outs] if single else outs
    shapes = [s if isinstance(s, jax.ShapeDtypeStruct) else jax.ShapeDtypeStruct(s, f32) for s in shapes]
    res = pl.pallas_call(
        kernel,
        out_shape=shapes,
        in_specs=[SMEM] * smem + [VMEM] * (len(ins) - smem),
        out_specs=[VMEM] * len(shapes),
        scratch_shapes=list(scratch),
        compiler_params=pltpu.CompilerParams(vmem_limit_bytes=limit * 1024 * 1024),
        cost_estimate=pl.CostEstimate(
            flops=int(us * 1e9), bytes_accessed=int(us * 1e6), transcendentals=0
        ),
    )(*ins)
    return res[0] if single else res


def shift(x, axis, by):
    n = lax.axis_size(axis)
    return lax.ppermute(x, axis, [(i, (i + by) % n) for i in range(n)])


def swap_sides(slabs):
    xhi, xlo, yhi, ylo = slabs
    return shift(xhi, "gx", 1), shift(xlo, "gx", -1), shift(yhi, "gy", 1), shift(ylo, "gy", -1)


def swap_corners(xlo, xhi, widths):
    shape = (corner_rows(widths), 128)
    yhi, ylo = call(functools.partial(corner_kernel, widths), [shape] * 2, [xlo, xhi], us=0.3)
    return shift(yhi, "gy", 1), shift(ylo, "gy", -1)


def on_device(load_index, load_table, toughness, clamp_mask, load_mask, crack_mask):
    home = lax.axis_index("section").astype(jnp.int32)
    nx, ny = lax.axis_size("gx"), lax.axis_size("gy")
    place = jnp.stack(
        [
            lax.axis_index("gx").astype(jnp.int32),
            lax.axis_index("gy").astype(jnp.int32),
            jnp.int32(nx),
            jnp.int32(ny),
        ]
    )
    vector = lax.dynamic_slice(load_table, (load_index[0], 0), (1, 3)).reshape(3)
    masks = lax.optimization_barrier(jnp.stack([load_mask, clamp_mask, crack_mask]))
    widths = mask_widths()
    kept, *slabs = call(
        first_pack_kernel, [(1, B, B, 128)] + [(slab_rows(widths), 128)] * 4,
        [masks, toughness], us=0.5,
    )
    received = swap_sides(slabs)
    corners = swap_corners(received[0], received[1], widths)
    sides = tuple(sorted({h for h in T_HALO if h}, reverse=True))
    ext = (ROWS, 128)
    made = call(
        functools.partial(first_kernel, sides),
        [(12,) + ext, ext, ext, ext, ext] + [(rows_of(h), 128) for h in sides],
        [place, vector, masks, kept, *received, *corners], [pltpu.VMEM(ext, f32)], smem=2, us=1.9,
    )
    state, kinds = made[0], made[1:5]
    given = state
    by_halo = dict(zip(sides, made[5:]))
    by_halo[0] = toughness.reshape(B * B, 128)
    tough = []
    for r, h in enumerate(T_HALO):
        tough.append(by_halo[h] if r == 0 else shift(by_halo[h], "section", -r))
    sums = jnp.zeros((1, 128), f32)
    for segment in SEGMENTS:
        g, begin, end = segment
        k = GROUPS[g]
        start = sum(GROUPS[:g])
        ins = [place, given, *kinds, sums, *tough[start + begin : start + end]]
        unpacks = g > 0 and begin == 0
        if unpacks:
            received = swap_sides(slabs)
            corners = swap_corners(received[0], received[1], state_widths(k))
            ins += [state, *received, *corners]
        else:
            ins.append(state)
        final = g == len(GROUPS) - 1 and end == k
        if final:
            outs = [(1, 3, B, B, 128), (1, B, B, 128), (nx * ny, 128)]
        elif end == k:
            n = slab_rows(state_widths(GROUPS[g + 1]))
            outs = [(4, B, B, 128)] + [(n, 128)] * 4 + [(1, 128)]
        else:
            outs = [(12,) + ext, (1, 128)]
        bufs = 2 if end - begin > 1 else 0
        scratch = [pltpu.VMEM(ext, f32)] * 3 + [pltpu.VMEM((12,) + ext, f32)] * bufs
        cost = sum((B + 4 * (k - 1 - j)) ** 2 * 0.007 for j in range(begin, end))
        res = call(
            functools.partial(sweep_kernel, segment), outs, ins, scratch,
            smem=1, us=cost, limit=4 + 8 * bufs,
        )
        if final:
            moved, damage, parts = res
        elif end == k:
            state, slabs, sums = res[0], res[1:5], res[5]
        else:
            state, sums = res
    parts = lax.all_to_all(parts, ("gx", "gy"), 0, 0, tiled=True)
    scale = 1.0 / (3.0 * B * B * 128 * nx * ny)
    parts = lax.dynamic_slice(parts, (0, ROUNDS - home), (nx * ny, ROUNDS))
    norms = jnp.sqrt(jnp.sum(parts, axis=0, keepdims=True) * scale)
    return moved, damage, norms


def solution(mesh):
    in_specs = (
        P("section"),
        P(),
        P("section", "gx", "gy", None),
        P("gx", "gy", None),
        P("gx", "gy", None),
        P("gx", "gy", None),
    )
    out_specs = (
        P("section", None, "gx", "gy", None),
        P("section", "gx", "gy", None),
        P("section", None),
    )
    return jax.shard_map(
        on_device, mesh=mesh, in_specs=in_specs, out_specs=out_specs, check_vma=False
    )
```

```python
import functools

import jax
import jax.numpy as jnp
from jax import lax
from jax.experimental import pallas as pl
from jax.experimental.pallas import tpu as pltpu
from jax.sharding import PartitionSpec as P


GROUPS = (4, 4)
B = 16
HALO = 2 * max(GROUPS) + 1
YP = B + 2 * HALO
ROWS = -(-(YP * (YP + 1) + 32) // 8) * 8

COS_THIRD = (
    1.000000008260009, -0.22222426779181312, -0.06576120509434145, -0.035390736331322045,
    -0.012547845736683551, -0.050373368401680454, 0.05848138776830297, -0.07087101496233855,
)
SIN_THIRD = (
    1.1547005306829978, 0.1069186220087089, 0.04565984619644209, 0.027903402002033718,
    0.00953945386696008, 0.04580735112208377, -0.054824704413705544, 0.06541734748383539,
)

SCALE = 16.0 ** (2.0 / 3.0)
ROUNDS = sum(GROUPS)
SEGMENTS = ((0, 0, 1), (0, 1, 2), (0, 2, 4), (1, 0, 4))
PLACES = [(g, j) for g, k in enumerate(GROUPS) for j in range(k)]
T_HALO = [2 * (GROUPS[g] - 1 - j) for g, j in PLACES]
T_MAX = max(T_HALO)
VMEM = pl.BlockSpec(memory_space=pltpu.VMEM)
SMEM = pl.BlockSpec(memory_space=pltpu.SMEM)
f32 = jnp.float32


def rows_of(h):
    side = B + 2 * h
    return side * side if h == 0 else -(-(side * side + 8) // 8) * 8


def mask_widths():
    k = GROUPS[0]
    return (2 * k + 1, 2 * k - 1, 2 * k, T_MAX)


def state_widths(k):
    return (2 * k + 1,) * 3 + (2 * k,)


def tri(h):
    return h * (h - 1) // 2


def slab_rows(widths):
    return B * sum(widths)


def corner_rows(widths):
    return -(-sum(2 * tri(h) for h in widths) // 8) * 8


def pieces(n):
    return [(s, min(8, n - s)) for s in range(0, n, 8)]


def pack_slabs(readers, widths, outs):
    xhi, xlo, yhi, ylo = outs
    off = 0
    for read, w in zip(readers, widths):
        for l in range(w):
            for s, n in pieces(B):
                xhi[pl.ds(off + l * B + s, n), :] = read(B - w + l, s, n)
                xlo[pl.ds(off + l * B + s, n), :] = read(l, s, n)
        for x in range(B):
            for s, n in pieces(w):
                yhi[pl.ds(off + x * w + s, n), :] = read(x, B - w + s, n)
                ylo[pl.ds(off + x * w + s, n), :] = read(x, s, n)
        off += B * w


def corner_kernel(widths, xlo, xhi, yhi, ylo):
    off = o = 0
    for h in widths:
        for slab, layer in ((xlo, lambda a: h - a), (xhi, lambda a: a - 1)):
            for a in range(1, h):
                n = h - a
                base = off + layer(a) * B
                yhi[pl.ds(o, n), :] = slab[pl.ds(base + B - n, n), :]
                ylo[pl.ds(o, n), :] = slab[pl.ds(base, n), :]
                o += n
        off += B * h


def unpack(own, slabs, corners, widths, edges, stores):
    xlo, xhi, ylo, yhi = slabs
    clo, chi = corners
    exlo, exhi, eylo, eyhi = edges
    off = o = 0
    for f, h in enumerate(widths):
        put = stores[f]
        for x in range(B):
            for s, n in pieces(B):
                put(x, s, own[f](x, s, n), None)
        for l in range(h):
            for s, n in pieces(B):
                put(l - h, s, xlo[pl.ds(off + l * B + s, n), :], exlo)
                put(B + l, s, xhi[pl.ds(off + l * B + s, n), :], exhi)
        for x in range(B):
            for s, n in pieces(h):
                put(x, s - h, ylo[pl.ds(off + x * h + s, n), :], eylo)
                put(x, B + s, yhi[pl.ds(off + x * h + s, n), :], eyhi)
        for side, edge in ((0, exlo), (1, exhi)):
            for a in range(1, h):
                n = h - a
                x = -a if side == 0 else B + a - 1
                put(x, -n, clo[pl.ds(o, n), :], jnp.logical_or(edge, eylo))
                put(x, B, chi[pl.ds(o, n), :], jnp.logical_or(edge, eyhi))
                o += n
        off += B * h


def edges_of(place):
    gx, gy = place[0], place[1]
    return gx == 0, gx == place[2] - 1, gy == 0, gy == place[3] - 1


def first_pack_kernel(masks, tough, kept, *outs):
    kept[...] = tough[...]
    pack_slabs(own_readers(masks, tough), mask_widths(), outs)


def own_readers(masks, tough):
    readers = [lambda x, y, n, f=f: masks[f, x, pl.ds(y, n), :].astype(f32) for f in range(3)]
    return readers + [lambda x, y, n: tough[0, x, pl.ds(y, n), :]]


def row(x, y):
    return (x + HALO) * YP + y + HALO


def first_kernel(
    sides, place, vector, masks, own_tough, xlo, xhi, ylo, yhi, clo, chi,
    state, fix, least, most, own_free, *rest,
):
    *tough_outs, ld = rest
    w = [vector[i] for i in range(3)]
    edges = edges_of(place)

    def choose(outside, value, other):
        return value if outside is None else jnp.where(outside, other, value)

    def put_clamp(x, y, v, outside):
        at = pl.ds(row(x, y), v.shape[0])
        v = jnp.maximum(choose(outside, v, 1.0), ld[at, :])
        fix[at, :] = v
        if outside is None:
            own_free[at, :] = 1.0 - v

    def put_load(x, y, v, outside):
        v = choose(outside, v, 0.0)
        at = pl.ds(row(x, y), v.shape[0])
        ld[at, :] = v
        above, below = up(v), down(v)
        for i in range(3):
            state[i, at, :] = v * w[i]
            state[4 + i, at, :] = above * w[i]
            state[7 + i, at, :] = below * w[i]

    def put_crack(x, y, v, outside):
        at = pl.ds(row(x, y), v.shape[0])
        v = choose(outside, v, 0.0)
        least[at, :] = v
        most[at, :] = choose(outside, jnp.ones_like(v), 0.0)
        put_state(state, 3, at, v)

    def put_tough(x, y, v, outside):
        n = v.shape[0]
        for ref, h in zip(tough_outs, sides):
            lo, hi = max(y, -h), min(y + n, B + h)
            if -h <= x < B + h and lo < hi:
                at = (x + h) * (B + 2 * h) + lo + h
                ref[pl.ds(at, hi - lo), :] = v[lo - y : hi - y]

    own_free[...] = jnp.zeros_like(own_free)
    unpack(
        own_readers(masks, own_tough), (xlo, xhi, ylo, yhi), (clo, chi), mask_widths(), edges,
        (put_load, put_clamp, put_crack, put_tough),
    )


def horner(coefs, w):
    acc = w * coefs[-1] + coefs[-2]
    for c in coefs[-3::-1]:
        acc = acc * w + c
    return acc


def up(v, outside=0.0):
    lane = lax.broadcasted_iota(jnp.int32, v.shape, 1)
    return jnp.where(lane == 127, outside, pltpu.roll(v, 127, 1))


def down(v, outside=0.0):
    lane = lax.broadcasted_iota(jnp.int32, v.shape, 1)
    return jnp.where(lane == 0, outside, pltpu.roll(v, 1, 1))


def put_state(ref, f, at, v):
    ref[f, at, :] = v
    plus, minus = ((4 + f, 7 + f) if f < 3 else (10, 11))
    ref[plus, at, :] = up(v)
    ref[minus, at, :] = down(v)


def sweep(src, dst, half, flow, flow_z, given, fix, least, most, own_free, tough, left):
    hd = 2 * left
    hm = hd + 1

    def chunks(h, i):
        base = i * YP + HALO - h
        return [base + 8 * t for t in range(-(-(B + 2 * h) // 8))]

    def flow_row(i):
        for r in chunks(hd + 2, i):
            at = pl.ds(r, 8)
            keep = 1.0 - src[3, at, :]
            h = keep * keep * 0.5 + 0.0005
            div = (
                (src[0, pl.ds(r + YP, 8), :] - src[0, pl.ds(r - YP, 8), :])
                + (src[1, pl.ds(r + 1, 8), :] - src[1, pl.ds(r - 1, 8), :])
                + (src[6, at, :] - src[9, at, :])
            )
            half[at, :] = h
            flow[at, :] = h * div * most[at, :]

    def turned_flow(i):
        out = []
        for r in chunks(hm, i):
            at = pl.ds(r, 8)
            v = flow[at, :]
            out.append((at, up(v) - down(v)))
        return out

    def put_flow_z(done):
        for at, v in done:
            flow_z[at, :] = v

    def turned(ref, fields, h, i):
        out = []
        for r in chunks(h, i):
            at = pl.ds(r, 8)
            for f in fields:
                v = ref[f, at, :]
                plus, minus = ((4 + f, 7 + f) if f < 3 else (10, 11))
                out.append((plus, at, up(v)))
                out.append((minus, at, down(v)))
        return out

    def put_turned(ref, done):
        for f, at, v in done:
            ref[f, at, :] = v

    def half_of(d):
        keep = 1.0 - d
        return keep * keep * 0.5 + 0.0005

    def moved_row(i, acc):
        for r in chunks(hd + 1, i):
            at = pl.ds(r, 8)
            around = [pl.ds(r + d, 8) for d in (YP, -YP, 1, -1)]
            h0 = half[at, :]
            hn = [half[a, :] for a in around] + [half_of(src[10, at, :]), half_of(src[11, at, :])]
            pairs = [hn[0] + hn[1], hn[2] + hn[3], hn[4] + hn[5]]
            weight = 6.0 * h0 + (pairs[0] + pairs[1] + pairs[2])
            faces = [h0 + n for n in hn]
            slope = [
                flow[around[0], :] - flow[around[1], :],
                flow[around[2], :] - flow[around[3], :],
                flow_z[at, :],
            ]
            is_fixed = fix[at, :] > 0.5
            squares = None
            for c in range(3):
                u0 = src[c, at, :]
                un = [src[c, a, :] for a in around] + [src[4 + c, at, :], src[7 + c, at, :]]
                res = slope[c] - weight * u0
                for f, n in zip(faces, un):
                    res = res + f * n
                relaxed = u0 + (res * 0.6) / (weight + pairs[c])
                dst[c, at, :] = jnp.where(is_fixed, given[c, at, :], relaxed)
                squares = res * res if squares is None else squares + res * res
            acc = acc + jnp.where(own_free[at, :] > 0.5, squares, 0.0)
        return acc

    def damage_row(i):
        for t, r in enumerate(chunks(hd, i)):
            at = pl.ds(r, 8)
            g = [
                (
                    dst[k, pl.ds(r + YP, 8), :] - dst[k, pl.ds(r - YP, 8), :],
                    dst[k, pl.ds(r + 1, 8), :] - dst[k, pl.ds(r - 1, 8), :],
                    dst[4 + k, at, :] - dst[7 + k, at, :],
                )
                for k in range(3)
            ]
            total = g[0][0] + g[1][1] + g[2][2]
            third = total * (1.0 / 3.0)
            dx, dy, dz = g[0][0] - third, g[1][1] - third, g[2][2] - third
            xy, xz, yz = g[0][1] + g[1][0], g[0][2] + g[2][0], g[1][2] + g[2][1]
            xy2, xz2, yz2 = xy * xy, xz * xz, yz * yz
            spread = (dx * dx + dy * dy + dz * dz) + 0.5 * (xy2 + xz2 + yz2)
            det = dx * dy * dz + 0.25 * (xy * xz * yz - (dx * yz2 + dy * xz2 + dz * xy2))
            s6 = spread * (1.0 / 24.0)
            inv = lax.rsqrt(spread * (SCALE / 24.0) + 1e-08 * SCALE)
            ratio = det * (inv * inv * inv)
            radius = s6 * lax.rsqrt(jnp.maximum(s6, 1e-37))
            wq = jnp.maximum(0.5 - 0.5 * jnp.abs(ratio), 0.0)
            cos = horner(COS_THIRD, wq)
            sin = (wq * lax.rsqrt(jnp.maximum(wq, 1e-37))) * horner(SIN_THIRD, wq)
            signed = jnp.where(ratio < 0.0, -radius, radius)
            a, b = signed * cos, signed * sin
            mean = total * (1.0 / 6.0)
            l1, rest = mean + 2.0 * a, mean - a
            p1 = jnp.maximum(l1, 0.0)
            p2 = jnp.maximum(rest + b, 0.0)
            p3 = jnp.maximum(rest - b, 0.0)
            trace = jnp.maximum(total, 0.0)
            psi2 = 0.25 * (trace * trace) + 2.0 * (p1 * p1 + p2 * p2 + p3 * p3)
            beside = (
                (src[3, pl.ds(r + YP, 8), :] + src[3, pl.ds(r - YP, 8), :])
                + (src[3, pl.ds(r + 1, 8), :] + src[3, pl.ds(r - 1, 8), :])
                + (src[10, at, :] + src[11, at, :])
            )
            gc = tough[pl.ds((i - (HALO - hd)) * (B + 2 * hd) + 8 * t, 8), :]
            new = (psi2 + gc * beside) / (psi2 + 7.0 * gc)
            dst[3, at, :] = jnp.minimum(jnp.maximum(new, least[at, :]), most[at, :])

    def step(i, acc, damaged):
        later = turned(dst, range(3), hd, i - 1)
        if damaged and left:
            later += turned(dst, (3,), hd - 1, i - 3)
        z_later = turned_flow(i + 1)
        flow_row(i + 2)
        acc = moved_row(i, acc)
        if damaged:
            damage_row(i - 2)
        put_turned(dst, later)
        put_flow_z(z_later)
        return acc

    low, high = HALO - hm, HALO + B + hm
    for i in (low - 1, low, low + 1):
        flow_row(i)
    put_flow_z(turned_flow(low))
    acc = lax.fori_loop(
        low, low + 3, lambda i, c: step(i, c, False), jnp.zeros((8, 128), f32)
    )
    acc = lax.fori_loop(low + 3, high, lambda i, c: step(i, c, True), acc)
    later = turned(dst, (3,), hd - 1, high - 3) if left else ()
    damage_row(high - 2)
    put_turned(dst, later)
    return acc


def add_sum(sums, acc, r):
    lane = lax.broadcasted_iota(jnp.int32, (1, 128), 1)
    return jnp.where(lane % ROUNDS == r, jnp.sum(acc), sums)


def sweep_kernel(segment, *refs):
    group, begin, end = segment
    k = GROUPS[group]
    final = group == len(GROUPS) - 1 and end == k
    refs = list(refs)

    def take(n):
        out = refs[:n]
        del refs[:n]
        return out

    place, given, fix, least, most, own_free, sums_in = take(7)
    tough = take(end - begin)
    unpacks = group > 0 and begin == 0
    if unpacks:
        state, xlo, xhi, ylo, yhi, clo, chi = take(7)
    else:
        (src,) = take(1)
    if final:
        moved_out, damage_out = take(2)
    elif end == k:
        (state_out,) = take(1)
        slab_outs = take(4)
    else:
        (wide_out,) = take(1)
    (sums_out,) = take(1)
    half, flow, flow_z, *bufs = refs
    if unpacks:
        src = bufs[1]

        def own(f):
            return lambda x, y, n: state[f, x, pl.ds(y, n), :]

        def put(f):
            def one(x, y, v, outside):
                v = v if outside is None else jnp.where(outside, 0.0, v)
                put_state(src, f, pl.ds(row(x, y), v.shape[0]), v)

            return one

        unpack(
            [own(f) for f in range(4)], (xlo, xhi, ylo, yhi), (clo, chi), state_widths(k),
            edges_of(place), [put(f) for f in range(4)],
        )
    sums = sums_in[...]
    start = sum(GROUPS[:group])
    for j in range(begin, end):
        dst = wide_out if j == end - 1 and end < k else bufs[j % 2]
        acc = sweep(
            src, dst, half, flow, flow_z, given, fix, least, most, own_free, tough[j - begin],
            k - 1 - j,
        )
        sums = add_sum(sums, acc, start + j)
        src = dst
    if final:
        for x in range(B):
            for s, n in pieces(B):
                at = pl.ds(row(x, s), n)
                for c in range(3):
                    moved_out[0, c, x, pl.ds(s, n), :] = src[c, at, :]
                damage_out[0, x, pl.ds(s, n), :] = src[3, at, :]
    elif end == k:
        for f in range(4):
            for x in range(B):
                for s, n in pieces(B):
                    state_out[f, x, pl.ds(s, n), :] = src[f, pl.ds(row(x, s), n), :]
        readers = [(lambda x, y, n, f=f: src[f, pl.ds(row(x, y), n), :]) for f in range(4)]
        pack_slabs(readers, state_widths(GROUPS[group + 1]), slab_outs)
    sums_out[...] = jnp.broadcast_to(sums, sums_out.shape)


def call(kernel, outs, ins, scratch=(), smem=0, us=1.0, limit=4):
    single = isinstance(outs, tuple)
    shapes = [outs] if single else outs
    shapes = [s if isinstance(s, jax.ShapeDtypeStruct) else jax.ShapeDtypeStruct(s, f32) for s in shapes]
    res = pl.pallas_call(
        kernel,
        out_shape=shapes,
        in_specs=[SMEM] * smem + [VMEM] * (len(ins) - smem),
        out_specs=[VMEM] * len(shapes),
        scratch_shapes=list(scratch),
        compiler_params=pltpu.CompilerParams(vmem_limit_bytes=limit * 1024 * 1024),
        cost_estimate=pl.CostEstimate(
            flops=int(us * 1e9), bytes_accessed=int(us * 1e6), transcendentals=0
        ),
    )(*ins)
    return res[0] if single else res


def shift(x, axis, by):
    n = lax.axis_size(axis)
    return lax.ppermute(x, axis, [(i, (i + by) % n) for i in range(n)])


def swap_sides(slabs):
    received = []
    for slab, axis, by in zip(slabs, ("gx", "gx", "gy", "gy"), (1, -1, 1, -1)):
        received.append(shift(slab, axis, by))
    return received


def swap_corners(xlo, xhi, widths):
    shape = (corner_rows(widths), 128)
    yhi, ylo = call(functools.partial(corner_kernel, widths), [shape] * 2, [xlo, xhi], us=0.3)
    return shift(yhi, "gy", 1), shift(ylo, "gy", -1)


def on_device(load_index, load_table, toughness, clamp_mask, load_mask, crack_mask):
    home = lax.axis_index("section").astype(jnp.int32)
    nx, ny = lax.axis_size("gx"), lax.axis_size("gy")
    place = jnp.stack(
        [
            lax.axis_index("gx").astype(jnp.int32),
            lax.axis_index("gy").astype(jnp.int32),
            jnp.int32(nx),
            jnp.int32(ny),
        ]
    )
    vector = lax.dynamic_slice(load_table, (load_index[0], 0), (1, 3)).reshape(3)
    masks = lax.optimization_barrier(jnp.stack([load_mask, clamp_mask, crack_mask]))
    widths = mask_widths()
    kept, *slabs = call(
        first_pack_kernel, [(1, B, B, 128)] + [(slab_rows(widths), 128)] * 4,
        [masks, toughness], us=0.5,
    )
    received = swap_sides(slabs)
    corners = swap_corners(received[0], received[1], widths)
    sides = tuple(sorted({h for h in T_HALO if h}, reverse=True))
    ext = (ROWS, 128)
    made = call(
        functools.partial(first_kernel, sides),
        [(12,) + ext, ext, ext, ext, ext] + [(rows_of(h), 128) for h in sides],
        [place, vector, masks, kept, *received, *corners], [pltpu.VMEM(ext, f32)], smem=2, us=1.9,
    )
    state, kinds = made[0], made[1:5]
    given = state
    by_halo = dict(zip(sides, made[5:]))
    by_halo[0] = toughness.reshape(B * B, 128)
    tough = []
    for r, h in enumerate(T_HALO):
        tough.append(by_halo[h] if r == 0 else shift(by_halo[h], "section", -r))
    sums = jnp.zeros((1, 128), f32)
    for segment in SEGMENTS:
        g, begin, end = segment
        k = GROUPS[g]
        start = sum(GROUPS[:g])
        ins = [place, given, *kinds, sums, *tough[start + begin : start + end]]
        unpacks = g > 0 and begin == 0
        if unpacks:
            received = swap_sides(slabs)
            corners = swap_corners(received[0], received[1], state_widths(k))
            ins += [state, *received, *corners]
        else:
            ins.append(state)
        final = g == len(GROUPS) - 1 and end == k
        if final:
            outs = [(1, 3, B, B, 128), (1, B, B, 128), (nx * ny, 128)]
        elif end == k:
            n = slab_rows(state_widths(GROUPS[g + 1]))
            outs = [(4, B, B, 128)] + [(n, 128)] * 4 + [(1, 128)]
        else:
            outs = [(12,) + ext, (1, 128)]
        bufs = 2 if end - begin > 1 else 0
        scratch = [pltpu.VMEM(ext, f32)] * 3 + [pltpu.VMEM((12,) + ext, f32)] * bufs
        cost = sum((B + 4 * (k - 1 - j)) ** 2 * 0.007 for j in range(begin, end))
        res = call(
            functools.partial(sweep_kernel, segment), outs, ins, scratch,
            smem=1, us=cost, limit=4 + 8 * bufs,
        )
        if final:
            moved, damage, parts = res
        elif end == k:
            state, slabs, sums = res[0], res[1:5], res[5]
        else:
            state, sums = res
    parts = lax.all_to_all(parts, ("gx", "gy"), 0, 0, tiled=True)
    scale = 1.0 / (3.0 * B * B * 128 * nx * ny)
    parts = lax.dynamic_slice(parts, (0, ROUNDS - home), (nx * ny, ROUNDS))
    norms = jnp.sqrt(jnp.sum(parts, axis=0, keepdims=True) * scale)
    return moved, damage, norms


def solution(mesh):
    in_specs = (
        P("section"),
        P(),
        P("section", "gx", "gy", None),
        P("gx", "gy", None),
        P("gx", "gy", None),
        P("gx", "gy", None),
    )
    out_specs = (
        P("section", None, "gx", "gy", None),
        P("section", "gx", "gy", None),
        P("section", None),
    )
    return jax.shard_map(
        on_device, mesh=mesh, in_specs=in_specs, out_specs=out_specs, check_vma=False
    )
```
